32 devices in a mesh: groups: 2 (over y), inner: 4 (over z), outer: 2 (over x), head: 2 (over core).
Axes of the slice: x: 2, y: 2, z: 4, core: 2. Of those that a mesh axis runs over, the one named last changes fastest.
Arguments:
- queries: bfloat16 [4, 512, 8, 128], P(('groups', 'outer'), 'inner', 'head'), parts along dimension 0, may hold values from -112 to 112
- keys: bfloat16 [4, 512, 128], P(('groups', 'outer'), 'inner'), parts along dimension 0, may hold values from -4 to 4
- values: bfloat16 [4, 512, 128], P(('groups', 'outer'), 'inner'), parts along dimension 0, may hold values from -6 to 6
- out: bfloat16 [4, 512, 8, 128], P(('groups', 'outer'), 'inner', 'head'), parts along dimension 0, may hold values from -6 to 6, as said below
- log_total: float32 [4, 8, 512], P(('groups', 'outer'), 'head', 'inner'), parts along dimension 0, as said below
- d_out: bfloat16 [4, 512, 8, 128], P(('groups', 'outer'), 'inner', 'head'), parts along dimension 0, may hold values from -6 to 6
- span_order: int32 [4, 8], P(('groups', 'outer')), parts along dimension 0, may hold values from 0 to 7, as said below
Outputs:
- grad_queries: bfloat16 [4, 512, 8, 128], P(('groups', 'outer'), 'inner', 'head'), parts along dimension 0
- grad_keys: bfloat16 [4, 512, 128], P(('groups', 'outer'), 'inner'), parts along dimension 0
- grad_values: bfloat16 [4, 512, 128], P(('groups', 'outer'), 'inner'), parts along dimension 0
The draws below stay inside these ranges and needn't reach their ends.
There are 2 independent parts, one for each index of `groups`. The reference program is written for one: setup_inputs(seed, part) draws one part's arguments, and reference() takes and returns one part's arrays. A program takes and returns all parts, laid end to end along the dimension named above; each array names one. Nothing has to cross between parts.
Inputs may be any that keep to these rules, and one draw needn't show every extreme that they name: `span_order`: each row is a permutation of 0 to 7. `out`: the causal softmax attention output of queries, keys and values in the order given by span_order, rounded to bfloat16. `log_total`: the log of the causal softmax total of each query row and head for the same inputs.
All inputs are finite; a program needn't handle non-finite values.
Results may differ from the reference program's by a relative error of at most 0.0054.
Values may be sent and summed in bfloat16 or wider, within the bound.
A program may use at most 64 MiB of HBM per device.

```python
import math
import jax
import jax.numpy as jnp
from jax import lax

HD = 128
GROUP_HEADS = 8
SPAN = 64
SEQ = 512
SPANS = 8
BATCH = 2


def layout_positions_drawn(block_order):
    rows = jnp.arange(SEQ, dtype=jnp.int32)
    tok_rows = 2 * SPAN
    owner = rows // tok_rows
    offset = rows % tok_rows
    span = block_order[(2 * owner + offset // SPAN).astype(jnp.int32)]
    return (span * SPAN + offset % SPAN).astype(jnp.int32)


def order_row(row_key):
    return jax.random.permutation(row_key, SPANS)


def base_draw(key):
    order_keys = jax.random.split(jax.random.fold_in(key, 100), BATCH)
    block_order = jax.vmap(order_row)(order_keys).astype(jnp.int32)
    base_keys = jnp.clip(jax.random.normal(jax.random.fold_in(key, 101), (BATCH, SEQ, HD), jnp.float32), -4.0, 4.0)
    base_queries = jnp.clip(jax.random.normal(jax.random.fold_in(key, 102), (BATCH, SEQ, GROUP_HEADS, HD), jnp.float32), -4.0, 4.0)
    base_values = jnp.clip(jax.random.normal(jax.random.fold_in(key, 106), (BATCH, SEQ, HD), jnp.float32), -6.0, 6.0)
    return (base_queries.astype(jnp.bfloat16), base_keys.astype(jnp.bfloat16), base_values.astype(jnp.bfloat16), block_order)


def forward_draw(key):
    queries, keys, values, block_order = base_draw(key)
    softmax_scale = 1.0 / math.sqrt(HD)
    tok_rows = 2 * SPAN

    def one_sequence(items):
        seq_queries, seq_keys, seq_values, seq_order = items
        positions = layout_positions_drawn(seq_order)
        key_float = seq_keys.astype(jnp.float32)
        value_float = seq_values.astype(jnp.float32)

        def one_block(block_index):
            start = (block_index * tok_rows).astype(jnp.int32)
            query_block = lax.dynamic_slice_in_dim(seq_queries, start, tok_rows, 0).astype(jnp.float32)
            query_pos = lax.dynamic_slice_in_dim(positions, start, tok_rows, 0)
            visible = positions[None, :] <= query_pos[:, None]
            scores = jnp.einsum('thd,ud->htu', query_block, key_float) * softmax_scale
            scores = jnp.where(visible[None], scores, -jnp.inf)
            row_max = jnp.max(scores, axis=-1, keepdims=True)
            block_total = row_max + jnp.log(jnp.sum(jnp.exp(scores - row_max), axis=-1, keepdims=True))
            probs = jnp.exp(scores - block_total)
            block_out = jnp.einsum('htu,ud->thd', probs, value_float)
            return (block_out, block_total[:, :, 0])
        outs, totals = lax.map(one_block, jnp.arange(SEQ // tok_rows, dtype=jnp.int32))
        seq_out = outs.reshape(SEQ, GROUP_HEADS, HD).astype(jnp.bfloat16)
        seq_total = jnp.transpose(totals, (1, 0, 2)).reshape(GROUP_HEADS, SEQ)
        return (seq_out, seq_total)
    return lax.map(one_sequence, (queries, keys, values, block_order))


def draw_queries(key, part):
    return base_draw(key)[0]


def draw_keys(key, part):
    return base_draw(key)[1]


def draw_values(key, part):
    return base_draw(key)[2]


def draw_span_order(key, part):
    return base_draw(key)[3]


def draw_out(key, part):
    return forward_draw(key)[0]


def draw_log_total(key, part):
    return forward_draw(key)[1].astype(jnp.float32)


def block_levels(rng, dims, shards, least, largest):
    factor_of = 1.0
    for position, blocks in shards:
        draws = jax.random.uniform(jax.random.fold_in(jax.random.fold_in(rng, 6), position), (blocks,), jnp.float32, least / len(shards), largest / len(shards))
        factor_of = factor_of * jnp.repeat(jnp.exp(draws), dims[position] // blocks).reshape((-1,) + (1,) * (len(dims) - 1 - position))
    return factor_of


def noise(rng, extent, deviation, reach, shards=(), kind=jnp.bfloat16):
    gain = block_levels(rng, extent, shards, -0.22, 0.18) if shards else 1.0
    values = jax.random.normal(rng, extent, jnp.float32) * deviation * gain
    return jnp.minimum(jnp.maximum(values, -reach), reach).astype(kind)


def setup_inputs(seed: int = 0, part: int = 0) -> dict:
    splits = jax.random.split(jax.random.key(seed), 8)
    part_splits = jax.random.split(jax.random.fold_in(splits[7], part), 8)
    return {
        "queries": draw_queries(jax.random.fold_in(jax.random.fold_in(splits[7], part), 71), part),
        "keys": draw_keys(jax.random.fold_in(jax.random.fold_in(splits[7], part), 71), part),
        "values": draw_values(jax.random.fold_in(jax.random.fold_in(splits[7], part), 71), part),
        "out": draw_out(jax.random.fold_in(jax.random.fold_in(splits[7], part), 71), part),
        "log_total": draw_log_total(jax.random.fold_in(jax.random.fold_in(splits[7], part), 71), part),
        "d_out": noise(part_splits[5], (BATCH, SEQ, GROUP_HEADS, HD), 1.0, 6.0, ((0, 2), (1, 4), (2, 2))),
        "span_order": draw_span_order(jax.random.fold_in(jax.random.fold_in(splits[7], part), 71), part),
    }


def layout_positions(block_order):
    rows = jnp.arange(SEQ, dtype=jnp.int32)
    tok_rows = 2 * SPAN
    owner = rows // tok_rows
    offset = rows % tok_rows
    span = block_order[(2 * owner + offset // SPAN).astype(jnp.int32)]
    return (span * SPAN + offset % SPAN).astype(jnp.int32)

def reference(queries, keys, values, out, log_total, d_out, span_order):
    softmax_scale = 1.0 / math.sqrt(HD)
    tok_rows = 2 * SPAN

    def one_sequence(items):
        seq_queries, seq_keys, seq_values, seq_out, seq_total, seq_grad, seq_order = items
        positions = layout_positions(seq_order)
        key_float = seq_keys.astype(jnp.float32)
        value_float = seq_values.astype(jnp.float32)

        def block(carry, block_index):
            key_total, value_total = carry
            start = (block_index * tok_rows).astype(jnp.int32)
            query_block = lax.dynamic_slice_in_dim(seq_queries, start, tok_rows, 0).astype(jnp.float32)
            grad_block = lax.dynamic_slice_in_dim(seq_grad, start, tok_rows, 0).astype(jnp.float32)
            out_block = lax.dynamic_slice_in_dim(seq_out, start, tok_rows, 0).astype(jnp.float32)
            total_block = lax.dynamic_slice_in_dim(seq_total, start, tok_rows, 1)
            query_pos = lax.dynamic_slice_in_dim(positions, start, tok_rows, 0)
            visible = positions[None, :] <= query_pos[:, None]
            scores = jnp.einsum('thd,ud->htu', query_block, key_float) * softmax_scale
            probs = jnp.exp(jnp.where(visible[None], scores - total_block[:, :, None], -jnp.inf))
            grad_probs = jnp.einsum('thd,ud->htu', grad_block, value_float)
            row_delta = jnp.transpose(lax.optimization_barrier(jnp.sum(out_block * grad_block, axis=-1)))[:, :, None]
            grad_scores = probs * (grad_probs - row_delta) * softmax_scale
            scores_half = lax.optimization_barrier(grad_scores.astype(jnp.bfloat16)).astype(jnp.float32)
            probs_half = lax.optimization_barrier(probs.astype(jnp.bfloat16)).astype(jnp.float32)
            query_grad = jnp.einsum('htu,ud->thd', scores_half, key_float).astype(jnp.bfloat16)
            key_total = key_total + jnp.einsum('htu,thd->ud', scores_half, query_block)
            value_total = value_total + jnp.einsum('htu,thd->ud', probs_half, grad_block)
            return ((key_total, value_total), query_grad)
        zeros = jnp.zeros((SEQ, HD), jnp.float32)
        (key_total, value_total), query_grads = lax.scan(block, (zeros, zeros), jnp.arange(SEQ // tok_rows, dtype=jnp.int32))
        grad_queries = query_grads.reshape(SEQ, GROUP_HEADS, HD)
        return (grad_queries, key_total.astype(jnp.bfloat16), value_total.astype(jnp.bfloat16))
    return lax.map(one_sequence, (queries, keys, values, out, log_total, d_out, span_order))
```

```python
import functools
import math

import jax
import jax.numpy as jnp
from jax import lax
from jax.experimental import pallas as pl
from jax.experimental.pallas import tpu as pltpu
from jax.sharding import PartitionSpec as P

MESH = pl.DeviceIdType.MESH
F32 = jnp.float32
BF16 = jnp.bfloat16
NT = (((1,), (1,)), ((), ()))
TN = (((0,), (0,)), ((), ()))
LOG2E = math.log2(math.e)


def dot(a, b, dims=(((1,), (0,)), ((), ()))):
    return lax.dot_general(a, b, dims, preferred_element_type=F32)


def kernel(
    n,
    heads,
    q_hbm,
    k_hbm,
    v_hbm,
    o_hbm,
    l_hbm,
    g_hbm,
    order_hbm,
    dq_ref,
    kv_ref,
    qs,
    gs,
    os_,
    ls,
    mine,
    kv,
    stat,
    ds_all,
    send_buf,
    recv_buf,
    dq_send,
    dq_recv,
    order,
    load_sem,
    pair_send,
    pair_recv,
    kv_send,
    kv_recv,
    grad_send,
    grad_recv,
    fin_send,
    fin_recv,
):
    me = lax.axis_index("inner")
    core = lax.axis_index("head")
    m = n // 2
    half, width = kv.shape[3], kv.shape[4]
    rows = qs.shape[1]
    scale = 1.0 / math.sqrt(width)
    partner = {"head": 1 - core}
    top, low = me // m, me % m

    def flip(value, bits):
        for k in range(m.bit_length()):
            if bits >> k & 1:
                value = value + (1 - 2 * ((value // 2**k) % 2)) * 2**k
        return value

    def flip_low(value, on):
        return value + on * (1 - 2 * (value % 2))

    inner_first = (low % 2 + top) % 2 * core if m > 1 else 0
    far_top = top + core - 2 * top * core
    slots = [flip_low(j, inner_first) if m > 1 else j for j in range(m)]
    peers = [
        far_top * m + (flip_low(flip(low, j), inner_first) if m > 1 else low)
        for j in range(m)
    ]

    barrier = pltpu.get_barrier_semaphore()

    def greet(inner, head):
        pl.semaphore_signal(
            barrier, inc=1, device_id={"inner": inner, "head": head}, device_id_type=MESH
        )

    @pl.when(core == 1)
    def _():
        for j in reversed(range(m)):
            greet(peers[j], 1)
        for j in range(m):
            greet(top * m + flip(low, j), 0)

    @pl.when(core == 0)
    def _():
        greet(me, 1)
        for j in range(1, m):
            greet(peers[j], 0)

    loads = [
        pltpu.make_async_copy(src, dst, load_sem.at[i])
        for i, (src, dst) in enumerate(
            (
                (k_hbm.at[0:half], mine.at[0, 0]),
                (v_hbm.at[0:half], mine.at[0, 1]),
                (k_hbm.at[half:], mine.at[1, 0]),
                (v_hbm.at[half:], mine.at[1, 1]),
                (q_hbm, qs.at[0]),
                (g_hbm, gs.at[0]),
                (o_hbm, os_),
                (l_hbm, ls),
                (order_hbm, order),
            )
        )
    ]
    for load in loads:
        load.start()

    @pl.when(core == 0)
    def _():
        for h in range(2):
            span = pl.ds(h * half, half)
            pltpu.make_async_copy(k_hbm.at[span], kv.at[0, h, 0], kv_recv.at[0, h]).start()
            pltpu.make_async_copy(v_hbm.at[span], kv.at[0, h, 1], kv_recv.at[0, h]).start()

    def kv_copy(j, h):
        return pltpu.make_async_remote_copy(
            src_ref=mine.at[h],
            dst_ref=kv.at[slots[j], h],
            send_sem=kv_send.at[j, h],
            recv_sem=kv_recv.at[slots[j], h],
            device_id={"inner": peers[j]},
            device_id_type=MESH,
        )

    for load in loads[:4]:
        load.wait()
    pl.semaphore_wait(barrier, jnp.where(core == 1, m + 1, n - 1))
    for j in reversed(range(1, m)):
        for h in range(2):
            kv_copy(j, h).start()

    @pl.when(core == 1)
    def _():
        for h in range(2):
            kv_copy(0, h).start()

    def pair_copy(i, src, dst):
        return pltpu.make_async_remote_copy(
            src_ref=src,
            dst_ref=dst,
            send_sem=pair_send.at[i],
            recv_sem=pair_recv.at[i],
            device_id=partner,
            device_id_type=MESH,
        )

    pair_copies = []
    for i, ref in enumerate((qs, gs)):
        loads[4 + i].wait()
        copy = pair_copy(i, ref.at[0], ref.at[1])
        copy.start()
        pair_copies.append(copy)
    loads[6].wait()
    loads[7].wait()

    toks = rows // heads
    col = lax.broadcasted_iota(jnp.int32, (toks, rows), 1)
    spread = jnp.where(
        col // heads == lax.broadcasted_iota(jnp.int32, (toks, rows), 0), 1.0, 0.0
    )
    head_of = lax.broadcasted_iota(jnp.int32, (heads, rows), 1) % heads
    pick = head_of == lax.broadcasted_iota(jnp.int32, (heads, rows), 0)
    ones = jnp.ones((8, width), BF16)
    total = jnp.dot(
        ls[...], spread, preferred_element_type=F32, precision=lax.Precision.HIGHEST
    )
    total = jnp.sum(jnp.where(pick, total, 0.0), axis=0, keepdims=True)
    prod = os_[...].astype(F32) * gs[0].astype(F32)
    high = prod.astype(BF16)
    rest = (prod - high.astype(F32)).astype(BF16)
    delta = dot(ones, high, NT) + dot(ones, rest, NT)
    stat[0, 0:1] = total * LOG2E
    stat[0, 1:2] = delta[0:1]
    copy = pair_copy(2, stat.at[0], stat.at[1])
    copy.start()
    pair_copies.append(copy)

    loads[8].wait()
    tok = (lax.broadcasted_iota(jnp.int32, (1, rows), 1)) // heads
    q_span = jnp.where(tok < half, order[2 * me], order[2 * me + 1])
    q_pos = q_span * half + tok % half
    q_span = jnp.concatenate([q_span, q_span], axis=1)
    q_pos = jnp.concatenate([q_pos, q_pos], axis=1)
    key_row = lax.broadcasted_iota(jnp.int32, (half, 1), 0)

    for copy in pair_copies:
        copy.wait_recv()
    totals = jnp.concatenate([stat[0, 0:1], stat[1, 0:1]], axis=1)
    deltas = jnp.concatenate([stat[0, 1:2], stat[1, 1:2]], axis=1)

    def block(j, h):
        k_span = order[2 * peers[j] + h]
        queries = qs[...].reshape(2 * rows, width)
        grads = gs[...].reshape(2 * rows, width)
        scores = dot(kv[slots[j], h, 0], queries, NT)
        grad_probs = dot(kv[slots[j], h, 1], grads, NT)
        if j == 0:
            visible = k_span * half + key_row <= q_pos
            probs = jnp.exp2(
                jnp.where(visible, scores * (scale * LOG2E) - totals, -jnp.inf)
            )
        else:
            shift = jnp.where(k_span < q_span, totals, jnp.inf)
            probs = jnp.exp2(scores * (scale * LOG2E) - shift)
        grad_scores = (probs * (grad_probs - deltas) * scale).astype(BF16)
        ds_all[j, h] = grad_scores
        yield 1, dot(probs.astype(BF16), grads)
        yield 0, dot(grad_scores, queries)

    def grad_copy(j, h, i):
        at = core * m + slots[j]
        return pltpu.make_async_remote_copy(
            src_ref=send_buf.at[j, h, i],
            dst_ref=recv_buf.at[at, h, i],
            send_sem=grad_send.at[j, h, i],
            recv_sem=grad_recv.at[at, h, i],
            device_id={"inner": peers[j], "head": 1},
            device_id_type=MESH,
        )

    for j in range(m):
        for h in range(2):
            kv_copy(j, h).wait_recv()
            for i, grad in block(j, h):
                send_buf[j, h, i] = grad.astype(BF16)
                grad_copy(j, h, i).start()

    def query_grad(i):
        total = None
        for j in range(m):
            for h in range(2):
                term = dot(
                    ds_all[j, h, :, i * rows : (i + 1) * rows], kv[slots[j], h, 0], TN
                )
                total = term if total is None else total + term
        return total

    dq_send[...] = query_grad(1)
    dq_copy = pair_copy(3, dq_send, dq_recv)
    dq_copy.start()
    own_grad = query_grad(0)
    dq_copy.wait_recv()
    dq_ref[...] = (own_grad + dq_recv[...]).astype(BF16)

    def fin_copy(h, i):
        span = kv_ref.at[i, pl.ds(h * half, half)]
        return pltpu.make_async_remote_copy(
            src_ref=span,
            dst_ref=span,
            send_sem=fin_send.at[h, i],
            recv_sem=fin_recv.at[h, i],
            device_id=partner,
            device_id_type=MESH,
        )

    @pl.when(core == 1)
    def _():
        for h in range(2):
            for i in (1, 0):
                total = None
                for d in range(n):
                    pltpu.make_async_remote_copy(
                        src_ref=send_buf.at[0, h, i],
                        dst_ref=recv_buf.at[d, h, i],
                        send_sem=grad_send.at[0, h, i],
                        recv_sem=grad_recv.at[d, h, i],
                        device_id=partner,
                        device_id_type=MESH,
                    ).wait_recv()
                    term = recv_buf[d, h, i].astype(F32)
                    total = term if total is None else total + term
                kv_ref[i, h * half : (h + 1) * half] = total.astype(BF16)
                fin_copy(h, i).start()
        for h in range(2):
            kv_copy(0, h).wait_send()
            for i in (1, 0):
                fin_copy(h, i).wait_send()

    for j in range(m):
        for h in range(2):
            if j:
                kv_copy(j, h).wait_send()
            for i in (1, 0):
                grad_copy(j, h, i).wait_send()
    for copy in pair_copies + [dq_copy]:
        copy.wait_send()

    @pl.when(core == 0)
    def _():
        for h in range(2):
            for i in (1, 0):
                fin_copy(h, i).wait_recv()


def store_kernel(dq_ref, kv_ref, dq_hbm, dk_hbm, dv_hbm, sem):
    pairs = ((dq_ref, dq_hbm), (kv_ref.at[0], dk_hbm), (kv_ref.at[1], dv_hbm))
    copies = [pltpu.make_async_copy(a, b, sem.at[i]) for i, (a, b) in enumerate(pairs)]
    for copy in copies:
        copy.start()
    for copy in copies:
        copy.wait()


def body(n, queries, keys, values, out, log_total, d_out, span_order):
    _, toks, heads, width = queries.shape
    rows = toks * heads
    half = toks // 2
    m = n // 2
    flat = lambda x: x.reshape(rows, width)
    anywhere = pl.BlockSpec(memory_space=pltpu.HBM)
    in_vmem = pl.BlockSpec(memory_space=pltpu.VMEM)
    dq, dkv = pl.pallas_call(
        functools.partial(kernel, n, heads),
        out_shape=(
            pltpu.VMEM((rows, width), BF16),
            pltpu.VMEM((2, toks, width), BF16),
        ),
        in_specs=[anywhere] * 7,
        out_specs=(in_vmem,) * 2,
        scratch_shapes=[
            pltpu.VMEM((2, rows, width), BF16),
            pltpu.VMEM((2, rows, width), BF16),
            pltpu.VMEM((rows, width), BF16),
            pltpu.VMEM((heads, toks), F32),
            pltpu.VMEM((2, 2, half, width), BF16),
            pltpu.VMEM((m, 2, 2, half, width), BF16),
            pltpu.VMEM((2, 8, rows), F32),
            pltpu.VMEM((m, 2, half, 2 * rows), BF16),
            pltpu.VMEM((m, 2, 2, half, width), BF16),
            pltpu.VMEM((n, 2, 2, half, width), BF16),
            pltpu.VMEM((rows, width), F32),
            pltpu.VMEM((rows, width), F32),
            pltpu.SMEM((span_order.shape[1],), jnp.int32),
            pltpu.SemaphoreType.DMA((9,)),
            pltpu.SemaphoreType.DMA((4,)),
            pltpu.SemaphoreType.DMA((4,)),
            pltpu.SemaphoreType.DMA((m, 2)),
            pltpu.SemaphoreType.DMA((m, 2)),
            pltpu.SemaphoreType.DMA((m, 2, 2)),
            pltpu.SemaphoreType.DMA((n, 2, 2)),
            pltpu.SemaphoreType.DMA((2, 2)),
            pltpu.SemaphoreType.DMA((2, 2)),
        ],
        compiler_params=pltpu.CompilerParams(collective_id=0, has_side_effects=True),
    )(
        flat(queries),
        keys[0],
        values[0],
        flat(out),
        log_total[0],
        flat(d_out),
        span_order[0],
    )
    dq, dk, dv = pl.pallas_call(
        store_kernel,
        out_shape=(
            jax.ShapeDtypeStruct((rows, width), BF16),
            jax.ShapeDtypeStruct((toks, width), BF16),
            jax.ShapeDtypeStruct((toks, width), BF16),
        ),
        in_specs=[in_vmem] * 2,
        out_specs=(anywhere,) * 3,
        scratch_shapes=[pltpu.SemaphoreType.DMA((3,))],
        compiler_params=pltpu.CompilerParams(vmem_limit_bytes=2**20),
    )(dq, dkv)
    return dq.reshape(queries.shape), dk[None], dv[None]


def solution(mesh):
    seq = ("groups", "outer")
    wide = P(seq, "inner", "head", None)
    narrow = P(seq, "inner", None)
    return jax.shard_map(
        functools.partial(body, mesh.shape["inner"]),
        mesh=mesh,
        in_specs=(wide, narrow, narrow, wide, P(seq, "head", "inner"), wide, P(seq, None)),
        out_specs=(wide, narrow, narrow),
        check_vma=False,
    )
```

```python
import functools
import math

import jax
import jax.numpy as jnp
from jax import lax
from jax.experimental import pallas as pl
from jax.experimental.pallas import tpu as pltpu
from jax.sharding import PartitionSpec as P

MESH = pl.DeviceIdType.MESH
F32 = jnp.float32
BF16 = jnp.bfloat16
NT = (((1,), (1,)), ((), ()))
TN = (((0,), (0,)), ((), ()))
LOG2E = math.log2(math.e)


def dot(a, b, dims=(((1,), (0,)), ((), ()))):
    return lax.dot_general(a, b, dims, preferred_element_type=F32)


def kernel(
    n,
    heads,
    q_hbm,
    k_hbm,
    v_hbm,
    o_hbm,
    l_hbm,
    g_hbm,
    order_hbm,
    dq_ref,
    kv_ref,
    qg,
    os_,
    ls,
    mine,
    kv,
    stat,
    ds_all,
    send_buf,
    recv_buf,
    dq_send,
    dq_recv,
    order,
    sem,
    pair_recv,
    kv_recv,
    grad_recv,
):
    me = lax.axis_index("inner")
    core = lax.axis_index("head")
    m = n // 2
    split = m + m // 2
    half, width = kv.shape[3], kv.shape[4]
    rows = qg.shape[2]
    scale = 1.0 / math.sqrt(width)
    partner = {"head": 1 - core}

    def chip(d):
        at = me
        for k in range(n.bit_length()):
            if d >> k & 1:
                at = at + (1 - 2 * ((me // 2**k) % 2)) * 2**k
        return at

    owners = [chip(j) + core * (chip(n - 1 - j) - chip(j)) for j in range(m)]

    barrier = pltpu.get_barrier_semaphore()

    def greet(inner, head):
        pl.semaphore_signal(
            barrier, inc=1, device_id={"inner": inner, "head": head}, device_id_type=MESH
        )

    @pl.when(core == 1)
    def _():
        for d in reversed(range(split, n)):
            greet(chip(d), 1)
        for d in reversed(range(m, split)):
            greet(chip(d), 0)
        greet(me, 0)

    @pl.when(core == 0)
    def _():
        for d in range(1, m):
            greet(chip(d), 0)
        greet(me, 1)

    loads = [
        pltpu.make_async_copy(src, dst, sem.at[i])
        for src, dst, i in (
            (k_hbm.at[0:half], mine.at[0, 0], 0),
            (v_hbm.at[0:half], mine.at[0, 1], 0),
            (k_hbm.at[half:], mine.at[1, 0], 0),
            (v_hbm.at[half:], mine.at[1, 1], 0),
            (q_hbm, qg.at[0, 0], 1),
            (g_hbm, qg.at[0, 1], 1),
            (o_hbm, os_, 2),
            (l_hbm, ls, 3),
            (order_hbm, order, 4),
        )
    ]
    for load in loads:
        load.start()

    @pl.when(core == 0)
    def _():
        for h in range(2):
            span = pl.ds(h * half, half)
            pltpu.make_async_copy(k_hbm.at[span], kv.at[0, h, 0], kv_recv.at[0, h]).start()
            pltpu.make_async_copy(v_hbm.at[span], kv.at[0, h, 1], kv_recv.at[0, h]).start()

    def remote(src, dst, send, recv, inner, head):
        return pltpu.make_async_remote_copy(
            src_ref=src,
            dst_ref=dst,
            send_sem=sem.at[send],
            recv_sem=recv,
            device_id={"inner": inner, "head": head},
            device_id_type=MESH,
        )

    def wait_bytes(ref, recv):
        remote(ref, ref, 0, recv, me, 1 - core).wait_recv()

    def wait_sent(ref, send):
        remote(ref, ref, send, pair_recv.at[0], me, 1 - core).wait_send()

    def kv_send(d):
        for h in range(2):
            slot = d if d < m else n - 1 - d
            remote(
                mine.at[h], kv.at[slot, h], 0, kv_recv.at[slot, h], chip(d), int(d >= m)
            ).start()

    wait_bytes(mine, sem.at[0])
    pl.semaphore_wait(barrier, jnp.where(core == 1, n - split + 1, split))

    @pl.when(core == 1)
    def _():
        for d in reversed(range(split, n)):
            kv_send(d)

    @pl.when(core == 0)
    def _():
        for d in reversed(range(1, split)):
            kv_send(d)

    wait_bytes(qg.at[0], sem.at[1])
    remote(qg.at[0], qg.at[1], 1, pair_recv.at[0], me, 1 - core).start()
    loads[6].wait()
    loads[7].wait()

    toks = rows // heads
    col = lax.broadcasted_iota(jnp.int32, (toks, rows), 1)
    spread = jnp.where(
        col // heads == lax.broadcasted_iota(jnp.int32, (toks, rows), 0), 1.0, 0.0
    )
    head_of = lax.broadcasted_iota(jnp.int32, (heads, rows), 1) % heads
    pick = head_of == lax.broadcasted_iota(jnp.int32, (heads, rows), 0)
    ones = jnp.ones((8, width), BF16)
    total = jnp.dot(
        ls[...], spread, preferred_element_type=F32, precision=lax.Precision.HIGHEST
    )
    total = jnp.sum(jnp.where(pick, total, 0.0), axis=0, keepdims=True)
    prod = os_[...].astype(F32) * qg[0, 1].astype(F32)
    high = prod.astype(BF16)
    rest = (prod - high.astype(F32)).astype(BF16)
    delta = dot(ones, high, NT) + dot(ones, rest, NT)
    stat[0, 0:1] = total * LOG2E
    stat[0, 1:2] = delta[0:1]
    remote(stat.at[0], stat.at[1], 2, pair_recv.at[1], me, 1 - core).start()

    loads[8].wait()
    tok = (lax.broadcasted_iota(jnp.int32, (1, rows), 1)) // heads
    q_span = jnp.where(tok < half, order[2 * me], order[2 * me + 1])
    q_pos = q_span * half + tok % half
    q_span = jnp.concatenate([q_span, q_span], axis=1)
    q_pos = jnp.concatenate([q_pos, q_pos], axis=1)
    key_row = lax.broadcasted_iota(jnp.int32, (half, 1), 0)

    with jax.named_scope("w_pair"):
        wait_bytes(qg.at[1], pair_recv.at[0])
        wait_bytes(stat.at[1], pair_recv.at[1])
    totals = jnp.concatenate([stat[0, 0:1], stat[1, 0:1]], axis=1)
    deltas = jnp.concatenate([stat[0, 1:2], stat[1, 1:2]], axis=1)

    def block(j, h):
        k_span = order[2 * owners[j] + h]
        queries = qg[:, 0].reshape(2 * rows, width)
        grads = qg[:, 1].reshape(2 * rows, width)
        scores = dot(kv[j, h, 0], queries, NT)
        grad_probs = dot(kv[j, h, 1], grads, NT)
        if j == 0:
            visible = k_span * half + key_row <= q_pos
            probs = jnp.exp2(
                jnp.where(visible, scores * (scale * LOG2E) - totals, -jnp.inf)
            )
        else:
            shift = jnp.where(k_span < q_span, totals, jnp.inf)
            probs = jnp.exp2(scores * (scale * LOG2E) - shift)
        grad_scores = (probs * (grad_probs - deltas) * scale).astype(BF16)
        ds_all[j, h] = grad_scores
        yield 1, dot(probs.astype(BF16), grads)
        yield 0, dot(grad_scores, queries)

    for j in range(m):
        for h in range(2):
            with jax.named_scope(f"w_kv{j}{h}"):
                wait_bytes(kv.at[j, h], kv_recv.at[j, h])
            with jax.named_scope(f"block{j}{h}"):
                for i, grad in block(j, h):
                    send_buf[j, h, i] = grad.astype(BF16)
                    at = j + core * (n - 1 - 2 * j)
                    remote(
                        send_buf.at[j, h, i],
                        recv_buf.at[at, h, i],
                        3,
                        grad_recv.at[at, h],
                        owners[j],
                        1,
                    ).start()

    def query_grad(i):
        total = None
        for j in range(m):
            for h in range(2):
                term = dot(
                    ds_all[j, h, :, i * rows : (i + 1) * rows], kv[j, h, 0], TN
                )
                total = term if total is None else total + term
        return total

    with jax.named_scope("dq"):
        dq_send[...] = query_grad(1)
        dq_copy = remote(dq_send, dq_recv, 4, pair_recv.at[2], me, 1 - core)
        dq_copy.start()
        own_grad = query_grad(0)
    with jax.named_scope("w_dq"):
        dq_copy.wait_recv()
    dq_ref[...] = (own_grad + dq_recv[...]).astype(BF16)

    with jax.named_scope("w_sends"):
        wait_sent(qg.at[0], 1)
        wait_sent(stat.at[0], 2)
        wait_sent(send_buf, 3)
        dq_copy.wait_send()

        @pl.when(core == 1)
        def _():
            wait_sent(recv_buf.at[0 : n - split], 0)

        @pl.when(core == 0)
        def _():
            if split > 1:
                wait_sent(recv_buf.at[1:split], 0)

    @pl.when(core == 1)
    def _():
        for h in range(2):
            total = [None, None]
            for d in range(n):
                with jax.named_scope(f"w_g{d}_{h}"):
                    wait_bytes(recv_buf.at[d, h], grad_recv.at[d, h])
                for i in range(2):
                    term = recv_buf[d, h, i].astype(F32)
                    total[i] = term if d == 0 else total[i] + term
            for i in range(2):
                span = kv_ref.at[i, pl.ds(h * half, half)]
                span[...] = total[i].astype(BF16)
                remote(span, span, 5, pair_recv.at[3], me, 0).start()
        with jax.named_scope("w_finsend"):
            wait_sent(kv_ref, 5)

    @pl.when(core == 0)
    def _():
        with jax.named_scope("w_fin"):
            wait_bytes(kv_ref, pair_recv.at[3])


def store_kernel(dq_ref, kv_ref, dq_hbm, dk_hbm, dv_hbm, sem):
    pairs = ((dq_ref, dq_hbm), (kv_ref.at[0], dk_hbm), (kv_ref.at[1], dv_hbm))
    copies = [pltpu.make_async_copy(a, b, sem.at[i]) for i, (a, b) in enumerate(pairs)]
    for copy in copies:
        copy.start()
    for copy in copies:
        copy.wait()


def body(n, queries, keys, values, out, log_total, d_out, span_order):
    _, toks, heads, width = queries.shape
    rows = toks * heads
    half = toks // 2
    m = n // 2
    flat = lambda x: x.reshape(rows, width)
    anywhere = pl.BlockSpec(memory_space=pltpu.HBM)
    in_vmem = pl.BlockSpec(memory_space=pltpu.VMEM)
    dq, dkv = pl.pallas_call(
        functools.partial(kernel, n, heads),
        out_shape=(
            pltpu.VMEM((rows, width), BF16),
            pltpu.VMEM((2, toks, width), BF16),
        ),
        in_specs=[anywhere] * 7,
        out_specs=(in_vmem,) * 2,
        scratch_shapes=[
            pltpu.VMEM((2, 2, rows, width), BF16),
            pltpu.VMEM((rows, width), BF16),
            pltpu.VMEM((heads, toks), F32),
            pltpu.VMEM((2, 2, half, width), BF16),
            pltpu.VMEM((m, 2, 2, half, width), BF16),
            pltpu.VMEM((2, 8, rows), F32),
            pltpu.VMEM((m, 2, half, 2 * rows), BF16),
            pltpu.VMEM((m, 2, 2, half, width), BF16),
            pltpu.VMEM((n, 2, 2, half, width), BF16),
            pltpu.VMEM((rows, width), F32),
            pltpu.VMEM((rows, width), F32),
            pltpu.SMEM((span_order.shape[1],), jnp.int32),
            pltpu.SemaphoreType.DMA((6,)),
            pltpu.SemaphoreType.DMA((4,)),
            pltpu.SemaphoreType.DMA((m, 2)),
            pltpu.SemaphoreType.DMA((n, 2)),
        ],
        compiler_params=pltpu.CompilerParams(collective_id=0, has_side_effects=True),
    )(
        flat(queries),
        keys[0],
        values[0],
        flat(out),
        log_total[0],
        flat(d_out),
        span_order[0],
    )
    dq, dk, dv = pl.pallas_call(
        store_kernel,
        out_shape=(
            jax.ShapeDtypeStruct((rows, width), BF16),
            jax.ShapeDtypeStruct((toks, width), BF16),
            jax.ShapeDtypeStruct((toks, width), BF16),
        ),
        in_specs=[in_vmem] * 2,
        out_specs=(anywhere,) * 3,
        scratch_shapes=[pltpu.SemaphoreType.DMA((3,))],
        compiler_params=pltpu.CompilerParams(vmem_limit_bytes=2**20),
    )(dq, dkv)
    return dq.reshape(queries.shape), dk[None], dv[None]


def solution(mesh):
    seq = ("groups", "outer")
    wide = P(seq, "inner", "head", None)
    narrow = P(seq, "inner", None)
    return jax.shard_map(
        functools.partial(body, mesh.shape["inner"]),
        mesh=mesh,
        in_specs=(wide, narrow, narrow, wide, P(seq, "head", "inner"), wide, P(seq, None)),
        out_specs=(wide, narrow, narrow),
        check_vma=False,
    )
```

```python
import functools
import math

import jax
import jax.numpy as jnp
from jax import lax
from jax.experimental import pallas as pl
from jax.experimental.pallas import tpu as pltpu
from jax.sharding import PartitionSpec as P

MESH = pl.DeviceIdType.MESH
F32 = jnp.float32
BF16 = jnp.bfloat16
NT = (((1,), (1,)), ((), ()))
TN = (((0,), (0,)), ((), ()))
LOG2E = math.log2(math.e)


def dot(a, b, dims=(((1,), (0,)), ((), ()))):
    return lax.dot_general(a, b, dims, preferred_element_type=F32)


def kernel(
    n,
    heads,
    q_hbm,
    k_hbm,
    v_hbm,
    o_hbm,
    l_hbm,
    g_hbm,
    order_hbm,
    dq_ref,
    kv_ref,
    qg,
    os_,
    ls,
    mine,
    kv,
    stat,
    ds_all,
    send_buf,
    recv_buf,
    part,
    dq_send,
    dq_recv,
    order,
    sem,
    pair_recv,
    kv_recv,
    grad_recv,
    entered,
):
    me = lax.axis_index("inner")
    core = lax.axis_index("head")
    m = n // 2
    split = m + m // 2
    toks, width = kv.shape[2], kv.shape[3]
    half = toks // 2
    rows = qg.shape[2]
    scale = 1.0 / math.sqrt(width)
    partner = {"head": 1 - core}

    def chip(d):
        at = me
        for k in range(n.bit_length()):
            if d >> k & 1:
                at = at + (1 - 2 * ((me // 2**k) % 2)) * 2**k
        return at

    owners = [chip(j) + core * (chip(n - 1 - j) - chip(j)) for j in range(m)]

    barrier = pltpu.get_barrier_semaphore()

    def greet(inner, head, when=None):
        def signal():
            pl.semaphore_signal(
                barrier, inc=1, device_id={"inner": inner, "head": head}, device_id_type=MESH
            )

        signal() if when is None else pl.when(when)(signal)

    @pl.when(core == 1)
    def _():
        greet(0, 1, me == 1)
        for d in reversed(range(split, n)):
            greet(chip(d), 1, chip(d) != 0)
        for d in reversed(range(m, split)):
            greet(chip(d), 0)
        greet(me, 0)

    @pl.when(core == 0)
    def _():
        for d in range(1, m):
            greet(chip(d), 0, chip(d) != 0)
        greet(me, 1)

    loads = [
        pltpu.make_async_copy(src, dst, sem.at[i])
        for src, dst, i in (
            (k_hbm, mine.at[0], 0),
            (v_hbm, mine.at[1], 0),
            (q_hbm, qg.at[0, 0], 1),
            (g_hbm, qg.at[0, 1], 1),
            (o_hbm, os_, 2),
            (l_hbm, ls, 3),
            (order_hbm, order, 4),
        )
    ]
    for load in loads:
        load.start()

    @pl.when(core == 0)
    def _():
        pltpu.make_async_copy(k_hbm, kv.at[0, 0], kv_recv.at[0, 0]).start()
        pltpu.make_async_copy(v_hbm, kv.at[0, 1], kv_recv.at[0, 1]).start()

    def remote(src, dst, send, recv, inner, head):
        return pltpu.make_async_remote_copy(
            src_ref=src,
            dst_ref=dst,
            send_sem=sem.at[send],
            recv_sem=recv,
            device_id={"inner": inner, "head": head},
            device_id_type=MESH,
        )

    def wait_bytes(ref, recv):
        remote(ref, ref, 0, recv, me, 1 - core).wait_recv()

    def wait_sent(ref, send):
        remote(ref, ref, send, pair_recv.at[0], me, 1 - core).wait_send()

    def slot_of(d):
        return d if d < m else n - 1 - d

    def kv_send(d):
        for i in range(2):
            place = (slot_of(d), i)
            remote(
                mine.at[i], kv.at[place], 0, kv_recv.at[place], chip(d), int(d >= m)
            ).start()

    wait_bytes(mine, sem.at[0])
    sent = jnp.where(
        me == 0,
        jnp.where(core == 1, 1, split - m),
        jnp.where(core == 1, n - split, split - 1),
    )
    pl.semaphore_wait(barrier, 1 + sent)

    @pl.when(me == 0)
    def _():
        @pl.when(core == 1)
        def _():
            for i in range(2):
                remote(mine.at[i], kv.at[m, i], 0, kv_recv.at[m, i], 1, 1).start()

    @pl.when(me != 0)
    def _():
        @pl.when(core == 1)
        def _():
            for d in reversed(range(split, n)):
                kv_send(d)

        @pl.when(core == 0)
        def _():
            @pl.when(me == 1)
            def _():
                pl.semaphore_signal(
                    entered, inc=1, device_id={"inner": me, "head": 1}, device_id_type=MESH
                )

            for d in range(1, m):
                kv_send(d)

    def middle_sends(when):
        @pl.when(jnp.logical_and(core == 0, when))
        def _():
            for d in range(m, split):
                kv_send(d)

    middle_sends(me != 1)

    wait_bytes(qg.at[0], sem.at[1])
    remote(qg.at[0], qg.at[1], 1, pair_recv.at[0], me, 1 - core).start()
    loads[4].wait()
    loads[5].wait()

    col = lax.broadcasted_iota(jnp.int32, (toks, rows), 1)
    spread = jnp.where(
        col // heads == lax.broadcasted_iota(jnp.int32, (toks, rows), 0), 1.0, 0.0
    )
    head_of = lax.broadcasted_iota(jnp.int32, (heads, rows), 1) % heads
    pick = head_of == lax.broadcasted_iota(jnp.int32, (heads, rows), 0)
    ones = jnp.ones((8, width), BF16)
    total = jnp.dot(
        ls[...], spread, preferred_element_type=F32, precision=lax.Precision.HIGHEST
    )
    total = jnp.sum(jnp.where(pick, total, 0.0), axis=0, keepdims=True)
    prod = os_[...].astype(F32) * qg[0, 1].astype(F32)
    high = prod.astype(BF16)
    rest = (prod - high.astype(F32)).astype(BF16)
    delta = dot(ones, high, NT) + dot(ones, rest, NT)
    stat[0, 0:1] = total * LOG2E
    stat[0, 1:2] = delta[0:1]
    remote(stat.at[0], stat.at[1], 2, pair_recv.at[1], me, 1 - core).start()

    loads[6].wait()

    relays = jnp.logical_and(me == 1, core == 1)

    @pl.when(relays)
    def _():
        def forward(i, c):
            place = (slot_of(c), i)
            remote(
                kv.at[m, i], kv.at[place], 4, kv_recv.at[place], c, int(c >= m)
            ).start()

        pl.semaphore_wait(entered, 1)
        for i in range(2):
            wait_bytes(kv.at[m, i], kv_recv.at[m, i])
            forward(i, n - 1)
            forward(i, 1)
        for c in (*range(split, n - 1), *range(2, m)):
            forward(0, c)
            forward(1, c)

    tok = (lax.broadcasted_iota(jnp.int32, (1, rows), 1)) // heads
    q_span = jnp.where(tok < half, order[2 * me], order[2 * me + 1])
    q_pos = q_span * half + tok % half
    q_span = jnp.concatenate([q_span, q_span], axis=1)
    q_pos = jnp.concatenate([q_pos, q_pos], axis=1)
    key_row = lax.broadcasted_iota(jnp.int32, (toks, 1), 0)

    with jax.named_scope("w_pair"):
        wait_bytes(qg.at[1], pair_recv.at[0])
        wait_bytes(stat.at[1], pair_recv.at[1])
    totals = jnp.concatenate([stat[0, 0:1], stat[1, 0:1]], axis=1)
    deltas = jnp.concatenate([stat[0, 1:2], stat[1, 1:2]], axis=1)

    def by_span(a, b):
        return jnp.where(key_row < half, a, b)

    def block(j):
        spans = [order[2 * owners[j] + h] for h in range(2)]
        queries = qg[:, 0].reshape(2 * rows, width)
        grads = qg[:, 1].reshape(2 * rows, width)
        with jax.named_scope(f"w_k{j}"):
            wait_bytes(kv.at[j, 0], kv_recv.at[j, 0])
        with jax.named_scope(f"dv{j}"):
            scores = dot(kv[j, 0], queries, NT)
            if j == 0:
                visible = by_span(*spans) * half + key_row % half <= q_pos
                probs = jnp.exp2(
                    jnp.where(visible, scores * (scale * LOG2E) - totals, -jnp.inf)
                )
            else:
                shifts = [jnp.where(k_span < q_span, totals, jnp.inf) for k_span in spans]
                probs = jnp.exp2(
                    jnp.concatenate(
                        [
                            scores[h * half : (h + 1) * half] * (scale * LOG2E) - shifts[h]
                            for h in range(2)
                        ]
                    )
                )
            yield 1, dot(probs.astype(BF16), grads)
        with jax.named_scope(f"w_v{j}"):
            wait_bytes(kv.at[j, 1], kv_recv.at[j, 1])
        with jax.named_scope(f"dk{j}"):
            grad_probs = dot(kv[j, 1], grads, NT)
            grad_scores = (probs * (grad_probs - deltas)).astype(BF16)
            ds_all[j] = grad_scores
            yield 0, dot(grad_scores, queries) * scale

    for j in range(m):
        at = j + core * (n - 1 - 2 * j)
        for i, grad in block(j):
            send_buf[j, i] = grad.astype(BF16)
            src, dst = send_buf.at[j, i], recv_buf.at[i, at]
            ready = grad_recv.at[i]
            if (j, i) == (0, 0):
                ready = grad_recv.at[2 * core]

                @pl.when(jnp.logical_and(core == 1, me == n - 1))
                def _():
                    remote(src, dst, 5, ready, 0, 0).start()

            remote(src, dst, 3, ready, owners[j], 1).start()

        if j == m - 1:
            middle_sends(me == 1)

    def query_grad(i):
        total = None
        for j in range(m):
            term = dot(ds_all[j, :, i * rows : (i + 1) * rows], kv[j, 0], TN)
            total = term if total is None else total + term
        return total * scale

    pl.when(relays)(lambda: wait_sent(recv_buf.at[:, 0 : n - split + m - 1], 4))

    with jax.named_scope("dq"):
        dq_send[...] = query_grad(1)
        dq_copy = remote(dq_send, dq_recv, 4, pair_recv.at[2], me, 1 - core)
        dq_copy.start()
        own_grad = query_grad(0)
    def sum_near():
        with jax.named_scope("w_near"):
            wait_bytes(recv_buf.at[0, 0 : n - 1], grad_recv.at[0])
        part[...] = sum(recv_buf[0, d].astype(F32) for d in range(n - 1))

    wait_sent(stat.at[0], 2)

    @pl.when(jnp.logical_and(core == 1, me == 0))
    def _():
        sum_near()
        remote(part, part, 2, pair_recv.at[4], me, 0).start()

    with jax.named_scope("w_dq"):
        dq_copy.wait_recv()
    dq_ref[...] = (own_grad + dq_recv[...]).astype(BF16)

    with jax.named_scope("w_sends"):
        wait_sent(qg.at[0], 1)
        wait_sent(send_buf, 3)
        dq_copy.wait_send()

        @pl.when(core == 1)
        def _():
            pl.when(me == 0)(lambda: wait_sent(mine, 0))
            pl.when(me != 0)(lambda: wait_sent(recv_buf.at[:, 0 : n - split], 0))

        @pl.when(jnp.logical_and(core == 0, me != 0))
        def _():
            wait_sent(recv_buf.at[:, 1:split], 0)

        @pl.when(jnp.logical_and(core == 0, me == 0))
        def _():
            wait_sent(recv_buf.at[:, m:split], 0)

    def sum_far():
        with jax.named_scope("w_far"):
            wait_bytes(recv_buf.at[0, n - 1], grad_recv.at[2])
        kv_ref[0] = (part[...] + recv_buf[0, n - 1].astype(F32)).astype(BF16)

    @pl.when(core == 1)
    def _():
        pl.when(me == n - 1)(lambda: wait_sent(send_buf.at[0, 0], 5))
        with jax.named_scope("w_v"):
            wait_bytes(recv_buf.at[1], grad_recv.at[1])
        kv_ref[1] = sum(recv_buf[1, d].astype(F32) for d in range(n)).astype(BF16)
        remote(kv_ref.at[1], kv_ref.at[1], 5, pair_recv.at[3], me, 0).start()
        pl.when(me != 0)(sum_near)
        sum_far()

        @pl.when(me != 0)
        def _():
            remote(kv_ref.at[0], kv_ref.at[0], 5, pair_recv.at[3], me, 0).start()
            wait_sent(kv_ref, 5)

        @pl.when(me == 0)
        def _():
            with jax.named_scope("w_finsend"):
                wait_sent(kv_ref.at[1], 5)
                wait_sent(part, 2)

    @pl.when(core == 0)
    def _():
        @pl.when(me != 0)
        def _():
            with jax.named_scope("w_fin"):
                wait_bytes(kv_ref, pair_recv.at[3])

        @pl.when(me == 0)
        def _():
            with jax.named_scope("w_part"):
                wait_bytes(part, pair_recv.at[4])
            sum_far()
            with jax.named_scope("w_finv"):
                wait_bytes(kv_ref.at[1], pair_recv.at[3])


def store_kernel(dq_ref, kv_ref, dq_hbm, dk_hbm, dv_hbm, sem):
    pairs = ((dq_ref, dq_hbm), (kv_ref.at[0], dk_hbm), (kv_ref.at[1], dv_hbm))
    copies = [pltpu.make_async_copy(a, b, sem.at[i]) for i, (a, b) in enumerate(pairs)]
    for copy in copies:
        copy.start()
    for copy in copies:
        copy.wait()


def body(n, queries, keys, values, out, log_total, d_out, span_order):
    _, toks, heads, width = queries.shape
    rows = toks * heads
    m = n // 2
    flat = lambda x: x.reshape(rows, width)
    anywhere = pl.BlockSpec(memory_space=pltpu.HBM)
    in_vmem = pl.BlockSpec(memory_space=pltpu.VMEM)
    dq, dkv = pl.pallas_call(
        functools.partial(kernel, n, heads),
        out_shape=(
            pltpu.VMEM((rows, width), BF16),
            pltpu.VMEM((2, toks, width), BF16),
        ),
        in_specs=[anywhere] * 7,
        out_specs=(in_vmem,) * 2,
        scratch_shapes=[
            pltpu.VMEM((2, 2, rows, width), BF16),
            pltpu.VMEM((rows, width), BF16),
            pltpu.VMEM((heads, toks), F32),
            pltpu.VMEM((2, toks, width), BF16),
            pltpu.VMEM((m + 1, 2, toks, width), BF16),
            pltpu.VMEM((2, 8, rows), F32),
            pltpu.VMEM((m, toks, 2 * rows), BF16),
            pltpu.VMEM((m, 2, toks, width), BF16),
            pltpu.VMEM((2, n, toks, width), BF16),
            pltpu.VMEM((toks, width), F32),
            pltpu.VMEM((rows, width), F32),
            pltpu.VMEM((rows, width), F32),
            pltpu.SMEM((span_order.shape[1],), jnp.int32),
            pltpu.SemaphoreType.DMA((6,)),
            pltpu.SemaphoreType.DMA((5,)),
            pltpu.SemaphoreType.DMA((m + 1, 2)),
            pltpu.SemaphoreType.DMA((3,)),
            pltpu.SemaphoreType.REGULAR,
        ],
        compiler_params=pltpu.CompilerParams(collective_id=0, has_side_effects=True),
    )(
        flat(queries),
        keys[0],
        values[0],
        flat(out),
        log_total[0],
        flat(d_out),
        span_order[0],
    )
    dq, dk, dv = pl.pallas_call(
        store_kernel,
        out_shape=(
            jax.ShapeDtypeStruct((rows, width), BF16),
            jax.ShapeDtypeStruct((toks, width), BF16),
            jax.ShapeDtypeStruct((toks, width), BF16),
        ),
        in_specs=[in_vmem] * 2,
        out_specs=(anywhere,) * 3,
        scratch_shapes=[pltpu.SemaphoreType.DMA((3,))],
        compiler_params=pltpu.CompilerParams(vmem_limit_bytes=2**20),
    )(dq, dkv)
    return dq.reshape(queries.shape), dk[None], dv[None]


def solution(mesh):
    seq = ("groups", "outer")
    wide = P(seq, "inner", "head", None)
    narrow = P(seq, "inner", None)
    return jax.shard_map(
        functools.partial(body, mesh.shape["inner"]),
        mesh=mesh,
        in_specs=(wide, narrow, narrow, wide, P(seq, "head", "inner"), wide, P(seq, None)),
        out_specs=(wide, narrow, narrow),
        check_vma=False,
    )
```

```python
import functools
import math

import jax
import jax.numpy as jnp
from jax import lax
from jax.experimental import pallas as pl
from jax.experimental.pallas import tpu as pltpu
from jax.sharding import PartitionSpec as P

MESH = pl.DeviceIdType.MESH
F32 = jnp.float32
BF16 = jnp.bfloat16
NT = (((1,), (1,)), ((), ()))
TN = (((0,), (0,)), ((), ()))
LOG2E = math.log2(math.e)


def dot(a, b, dims=(((1,), (0,)), ((), ()))):
    return lax.dot_general(a, b, dims, preferred_element_type=F32)


def kernel(
    n,
    heads,
    q_hbm,
    k_hbm,
    v_hbm,
    o_hbm,
    l_hbm,
    g_hbm,
    order_hbm,
    dq_ref,
    kv_ref,
    qg,
    os_,
    ls,
    mine,
    kv,
    stat,
    ds_all,
    send_buf,
    recv_buf,
    part,
    dq_send,
    dq_recv,
    order,
    sem,
    pair_recv,
    kv_recv,
    grad_recv,
    entered,
):
    me = lax.axis_index("inner")
    core = lax.axis_index("head")
    m = n // 2
    split = m + m // 2
    toks, width = kv.shape[2], kv.shape[3]
    half = toks // 2
    rows = qg.shape[2]
    scale = 1.0 / math.sqrt(width)
    partner = {"head": 1 - core}

    def chip(d):
        at = me
        for k in range(n.bit_length()):
            if d >> k & 1:
                at = at + (1 - 2 * ((me // 2**k) % 2)) * 2**k
        return at

    owners = [chip(j) + core * (chip(n - 1 - j) - chip(j)) for j in range(m)]

    barrier = pltpu.get_barrier_semaphore()

    def greet(inner, head, when=None):
        def signal():
            pl.semaphore_signal(
                barrier, inc=1, device_id={"inner": inner, "head": head}, device_id_type=MESH
            )

        signal() if when is None else pl.when(when)(signal)

    @pl.when(core == 1)
    def _():
        greet(0, 1, me == 1)
        for d in reversed(range(split, n)):
            greet(chip(d), 1, chip(d) != 0)
        for d in reversed(range(m, split)):
            greet(chip(d), 0)
        greet(me, 0)

    @pl.when(core == 0)
    def _():
        for d in range(1, m):
            greet(chip(d), 0, chip(d) != 0)
        greet(me, 1)

    loads = [
        pltpu.make_async_copy(src, dst, sem.at[i])
        for src, dst, i in (
            (k_hbm, mine.at[0], 0),
            (v_hbm, mine.at[1], 0),
            (q_hbm, qg.at[0, 0], 1),
            (g_hbm, qg.at[0, 1], 1),
            (o_hbm, os_, 2),
            (l_hbm, ls, 3),
            (order_hbm, order, 4),
        )
    ]
    for load in loads:
        load.start()

    @pl.when(core == 0)
    def _():
        pltpu.make_async_copy(k_hbm, kv.at[0, 0], kv_recv.at[0, 0]).start()
        pltpu.make_async_copy(v_hbm, kv.at[0, 1], kv_recv.at[0, 1]).start()

    def remote(src, dst, send, recv, inner, head):
        return pltpu.make_async_remote_copy(
            src_ref=src,
            dst_ref=dst,
            send_sem=sem.at[send],
            recv_sem=recv,
            device_id={"inner": inner, "head": head},
            device_id_type=MESH,
        )

    def wait_bytes(ref, recv):
        remote(ref, ref, 0, recv, me, 1 - core).wait_recv()

    def wait_sent(ref, send):
        remote(ref, ref, send, pair_recv.at[0], me, 1 - core).wait_send()

    def slot_of(d):
        return d if d < m else n - 1 - d

    def kv_send(d, parts=(0, 1)):
        for i in parts:
            place = (slot_of(d), i)
            remote(
                mine.at[i], kv.at[place], 0, kv_recv.at[place], chip(d), int(d >= m)
            ).start()

    wait_bytes(mine, sem.at[0])
    sent = jnp.where(
        me == 0,
        jnp.where(core == 1, 1, split - m),
        jnp.where(core == 1, n - split, split - 1),
    )
    pl.semaphore_wait(barrier, 1 + sent)

    @pl.when(me == 0)
    def _():
        @pl.when(core == 1)
        def _():
            for i in range(2):
                remote(mine.at[i], kv.at[m, i], 0, kv_recv.at[m, i], 1, 1).start()

    @pl.when(me != 0)
    def _():
        @pl.when(core == 1)
        def _():
            for d in reversed(range(split, n)):
                kv_send(d)

        @pl.when(core == 0)
        def _():
            @pl.when(me == 1)
            def _():
                pl.semaphore_signal(
                    entered, inc=1, device_id={"inner": me, "head": 1}, device_id_type=MESH
                )

            for d in range(1, m):
                kv_send(d)

    def middle_sends(when, parts=(0, 1)):
        @pl.when(jnp.logical_and(core == 0, when))
        def _():
            for d in range(m, split):
                kv_send(d, parts)

    middle_sends(me > 1)
    middle_sends(me == 0, (0,))

    wait_bytes(qg.at[0], sem.at[1])
    remote(qg.at[0], qg.at[1], 1, pair_recv.at[0], me, 1 - core).start()
    loads[4].wait()
    loads[5].wait()

    col = lax.broadcasted_iota(jnp.int32, (toks, rows), 1)
    spread = jnp.where(
        col // heads == lax.broadcasted_iota(jnp.int32, (toks, rows), 0), 1.0, 0.0
    )
    head_of = lax.broadcasted_iota(jnp.int32, (heads, rows), 1) % heads
    pick = head_of == lax.broadcasted_iota(jnp.int32, (heads, rows), 0)
    ones = jnp.ones((8, width), BF16)
    total = jnp.dot(
        ls[...], spread, preferred_element_type=F32, precision=lax.Precision.HIGHEST
    )
    total = jnp.sum(jnp.where(pick, total, 0.0), axis=0, keepdims=True)
    prod = os_[...].astype(F32) * qg[0, 1].astype(F32)
    high = prod.astype(BF16)
    rest = (prod - high.astype(F32)).astype(BF16)
    delta = dot(ones, high, NT) + dot(ones, rest, NT)
    stat[0, 0:1] = total * LOG2E
    stat[0, 1:2] = delta[0:1]
    remote(stat.at[0], stat.at[1], 2, pair_recv.at[1], me, 1 - core).start()

    loads[6].wait()

    relays = jnp.logical_and(me == 1, core == 1)

    @pl.when(relays)
    def _():
        def forward(i, c):
            place = (slot_of(c), i)
            remote(
                kv.at[m, i], kv.at[place], 4, kv_recv.at[place], c, int(c >= m)
            ).start()

        pl.semaphore_wait(entered, 1)
        for i in range(2):
            wait_bytes(kv.at[m, i], kv_recv.at[m, i])
            forward(i, n - 1)
            forward(i, 1)
        for c in (*range(split, n - 1), *range(2, m)):
            forward(0, c)
            forward(1, c)

    tok = (lax.broadcasted_iota(jnp.int32, (1, rows), 1)) // heads
    q_span = jnp.where(tok < half, order[2 * me], order[2 * me + 1])
    q_pos = q_span * half + tok % half
    q_span = jnp.concatenate([q_span, q_span], axis=1)
    q_pos = jnp.concatenate([q_pos, q_pos], axis=1)
    key_row = lax.broadcasted_iota(jnp.int32, (toks, 1), 0)

    with jax.named_scope("w_pair"):
        wait_bytes(qg.at[1], pair_recv.at[0])
        wait_bytes(stat.at[1], pair_recv.at[1])
    totals = jnp.concatenate([stat[0, 0:1], stat[1, 0:1]], axis=1)
    deltas = jnp.concatenate([stat[0, 1:2], stat[1, 1:2]], axis=1)

    def by_span(a, b):
        return jnp.where(key_row < half, a, b)

    def block(j):
        spans = [order[2 * owners[j] + h] for h in range(2)]
        queries = qg[:, 0].reshape(2 * rows, width)
        grads = qg[:, 1].reshape(2 * rows, width)
        with jax.named_scope(f"w_k{j}"):
            wait_bytes(kv.at[j, 0], kv_recv.at[j, 0])
        with jax.named_scope(f"dv{j}"):
            scores = dot(kv[j, 0], queries, NT)
            if j == 0:
                visible = by_span(*spans) * half + key_row % half <= q_pos
                probs = jnp.exp2(
                    jnp.where(visible, scores * (scale * LOG2E) - totals, -jnp.inf)
                )
            else:
                shifts = [jnp.where(k_span < q_span, totals, jnp.inf) for k_span in spans]
                probs = jnp.exp2(
                    jnp.concatenate(
                        [
                            scores[h * half : (h + 1) * half] * (scale * LOG2E) - shifts[h]
                            for h in range(2)
                        ]
                    )
                )
            yield 1, dot(probs.astype(BF16), grads)
        with jax.named_scope(f"w_v{j}"):
            wait_bytes(kv.at[j, 1], kv_recv.at[j, 1])
        with jax.named_scope(f"dk{j}"):
            grad_probs = dot(kv[j, 1], grads, NT)
            grad_scores = (probs * (grad_probs - deltas) * scale).astype(BF16)
            ds_all[j] = grad_scores
            yield 0, dot(grad_scores, queries)

    for j in range(m):
        at = j + core * (n - 1 - 2 * j)
        for i, grad in block(j):
            send_buf[j, i] = grad.astype(BF16)
            src, dst = send_buf.at[j, i], recv_buf.at[i, at]
            ready = grad_recv.at[i]
            if (j, i) == (0, 0):
                ready = grad_recv.at[2 * core]

                @pl.when(jnp.logical_and(core == 1, me == n - 1))
                def _():
                    remote(src, dst, 5, ready, 0, 0).start()

            remote(src, dst, 3, ready, owners[j], 1).start()
            if (j, i) == (0, 1):
                middle_sends(me == 0, (1,))
            if (j, i) == (m - 1, 1):
                middle_sends(me == 1)

    def query_grad(i):
        total = None
        for j in range(m):
            term = dot(ds_all[j, :, i * rows : (i + 1) * rows], kv[j, 0], TN)
            total = term if total is None else total + term
        return total

    pl.when(relays)(lambda: wait_sent(recv_buf.at[:, 0 : n - split + m - 1], 4))

    with jax.named_scope("dq"):
        dq_send[...] = query_grad(1)
        dq_copy = remote(dq_send, dq_recv, 4, pair_recv.at[2], me, 1 - core)
        dq_copy.start()
        own_grad = query_grad(0)
    def sum_near():
        with jax.named_scope("w_near"):
            wait_bytes(recv_buf.at[0, 0 : n - 1], grad_recv.at[0])
        part[...] = sum(recv_buf[0, d].astype(F32) for d in range(n - 1))

    wait_sent(stat.at[0], 2)

    @pl.when(jnp.logical_and(core == 1, me == 0))
    def _():
        sum_near()
        remote(part, part, 2, pair_recv.at[4], me, 0).start()

    with jax.named_scope("w_dq"):
        dq_copy.wait_recv()
    dq_ref[...] = (own_grad + dq_recv[...]).astype(BF16)

    with jax.named_scope("w_sends"):
        wait_sent(qg.at[0], 1)
        wait_sent(send_buf, 3)
        dq_copy.wait_send()

        @pl.when(core == 1)
        def _():
            pl.when(me == 0)(lambda: wait_sent(mine, 0))
            pl.when(me != 0)(lambda: wait_sent(recv_buf.at[:, 0 : n - split], 0))

        @pl.when(jnp.logical_and(core == 0, me != 0))
        def _():
            wait_sent(recv_buf.at[:, 1:split], 0)

        @pl.when(jnp.logical_and(core == 0, me == 0))
        def _():
            wait_sent(recv_buf.at[:, m:split], 0)

    def sum_far():
        with jax.named_scope("w_far"):
            wait_bytes(recv_buf.at[0, n - 1], grad_recv.at[2])
        kv_ref[0] = (part[...] + recv_buf[0, n - 1].astype(F32)).astype(BF16)

    @pl.when(core == 1)
    def _():
        pl.when(me == n - 1)(lambda: wait_sent(send_buf.at[0, 0], 5))
        with jax.named_scope("w_v"):
            wait_bytes(recv_buf.at[1], grad_recv.at[1])
        kv_ref[1] = sum(recv_buf[1, d].astype(F32) for d in range(n)).astype(BF16)
        remote(kv_ref.at[1], kv_ref.at[1], 5, pair_recv.at[3], me, 0).start()
        pl.when(me != 0)(sum_near)
        sum_far()

        @pl.when(me != 0)
        def _():
            remote(kv_ref.at[0], kv_ref.at[0], 5, pair_recv.at[3], me, 0).start()
            wait_sent(kv_ref, 5)

        @pl.when(me == 0)
        def _():
            with jax.named_scope("w_finsend"):
                wait_sent(kv_ref.at[1], 5)
                wait_sent(part, 2)

    @pl.when(core == 0)
    def _():
        @pl.when(me != 0)
        def _():
            with jax.named_scope("w_fin"):
                wait_bytes(kv_ref, pair_recv.at[3])

        @pl.when(me == 0)
        def _():
            with jax.named_scope("w_part"):
                wait_bytes(part, pair_recv.at[4])
            sum_far()
            with jax.named_scope("w_finv"):
                wait_bytes(kv_ref.at[1], pair_recv.at[3])


def store_kernel(dq_ref, kv_ref, dq_hbm, dk_hbm, dv_hbm, sem):
    pairs = ((dq_ref, dq_hbm), (kv_ref.at[0], dk_hbm), (kv_ref.at[1], dv_hbm))
    copies = [pltpu.make_async_copy(a, b, sem.at[i]) for i, (a, b) in enumerate(pairs)]
    for copy in copies:
        copy.start()
    for copy in copies:
        copy.wait()


def body(n, queries, keys, values, out, log_total, d_out, span_order):
    _, toks, heads, width = queries.shape
    rows = toks * heads
    m = n // 2
    flat = lambda x: x.reshape(rows, width)
    anywhere = pl.BlockSpec(memory_space=pltpu.HBM)
    in_vmem = pl.BlockSpec(memory_space=pltpu.VMEM)
    dq, dkv = pl.pallas_call(
        functools.partial(kernel, n, heads),
        out_shape=(
            pltpu.VMEM((rows, width), BF16),
            pltpu.VMEM((2, toks, width), BF16),
        ),
        in_specs=[anywhere] * 7,
        out_specs=(in_vmem,) * 2,
        scratch_shapes=[
            pltpu.VMEM((2, 2, rows, width), BF16),
            pltpu.VMEM((rows, width), BF16),
            pltpu.VMEM((heads, toks), F32),
            pltpu.VMEM((2, toks, width), BF16),
            pltpu.VMEM((m + 1, 2, toks, width), BF16),
            pltpu.VMEM((2, 8, rows), F32),
            pltpu.VMEM((m, toks, 2 * rows), BF16),
            pltpu.VMEM((m, 2, toks, width), BF16),
            pltpu.VMEM((2, n, toks, width), BF16),
            pltpu.VMEM((toks, width), F32),
            pltpu.VMEM((rows, width), F32),
            pltpu.VMEM((rows, width), F32),
            pltpu.SMEM((span_order.shape[1],), jnp.int32),
            pltpu.SemaphoreType.DMA((6,)),
            pltpu.SemaphoreType.DMA((5,)),
            pltpu.SemaphoreType.DMA((m + 1, 2)),
            pltpu.SemaphoreType.DMA((3,)),
            pltpu.SemaphoreType.REGULAR,
        ],
        compiler_params=pltpu.CompilerParams(collective_id=0, has_side_effects=True),
    )(
        flat(queries),
        keys[0],
        values[0],
        flat(out),
        log_total[0],
        flat(d_out),
        span_order[0],
    )
    dq, dk, dv = pl.pallas_call(
        store_kernel,
        out_shape=(
            jax.ShapeDtypeStruct((rows, width), BF16),
            jax.ShapeDtypeStruct((toks, width), BF16),
            jax.ShapeDtypeStruct((toks, width), BF16),
        ),
        in_specs=[in_vmem] * 2,
        out_specs=(anywhere,) * 3,
        scratch_shapes=[pltpu.SemaphoreType.DMA((3,))],
        compiler_params=pltpu.CompilerParams(vmem_limit_bytes=2**20),
    )(dq, dkv)
    return dq.reshape(queries.shape), dk[None], dv[None]


def solution(mesh):
    seq = ("groups", "outer")
    wide = P(seq, "inner", "head", None)
    narrow = P(seq, "inner", None)
    return jax.shard_map(
        functools.partial(body, mesh.shape["inner"]),
        mesh=mesh,
        in_specs=(wide, narrow, narrow, wide, P(seq, "head", "inner"), wide, P(seq, None)),
        out_specs=(wide, narrow, narrow),
        check_vma=False,
    )
```

```python
import functools
import math

import jax
import jax.numpy as jnp
from jax import lax
from jax.experimental import pallas as pl
from jax.experimental.pallas import tpu as pltpu
from jax.sharding import PartitionSpec as P

MESH = pl.DeviceIdType.MESH
F32 = jnp.float32
BF16 = jnp.bfloat16
NT = (((1,), (1,)), ((), ()))
TN = (((0,), (0,)), ((), ()))
LOG2E = math.log2(math.e)


def dot(a, b, dims=(((1,), (0,)), ((), ()))):
    return lax.dot_general(a, b, dims, preferred_element_type=F32)


def kernel(
    n,
    heads,
    q_hbm,
    k_hbm,
    v_hbm,
    o_hbm,
    l_hbm,
    g_hbm,
    order_hbm,
    dq_ref,
    kv_ref,
    qg,
    os_,
    ls,
    mine,
    kv,
    stat,
    ds_all,
    send_buf,
    recv_buf,
    part,
    dq_send,
    dq_recv,
    order,
    sem,
    pair_recv,
    kv_recv,
    grad_recv,
    entry,
    entered,
):
    me = lax.axis_index("inner")
    core = lax.axis_index("head")
    m = n // 2
    split = m + m // 2
    toks, width = kv.shape[2], kv.shape[3]
    half = toks // 2
    rows = qg.shape[2]
    scale = 1.0 / math.sqrt(width)
    partner = {"head": 1 - core}

    def chip(d):
        at = me
        for k in range(n.bit_length()):
            if d >> k & 1:
                at = at + (1 - 2 * ((me // 2**k) % 2)) * 2**k
        return at

    owners = [chip(j) + core * (chip(n - 1 - j) - chip(j)) for j in range(m)]

    barrier = pltpu.get_barrier_semaphore()

    def greet(inner, head, when=None):
        def signal():
            pl.semaphore_signal(
                barrier, inc=1, device_id={"inner": inner, "head": head}, device_id_type=MESH
            )

        signal() if when is None else pl.when(when)(signal)

    @pl.when(core == 1)
    def _():
        greet(0, 1, me == 1)
        for d in reversed(range(split, n)):
            greet(chip(d), 1, chip(d) != 0)
        for d in reversed(range(m, split)):
            greet(chip(d), 0, chip(d) != 0)
        greet(me, 0)

    @pl.when(core == 0)
    def _():
        for d in range(1, m):
            greet(chip(d), 0, chip(d) != 0)
        greet(me, 1)

    loads = [
        pltpu.make_async_copy(src, dst, sem.at[i])
        for src, dst, i in (
            (k_hbm, mine.at[0], 0),
            (v_hbm, mine.at[1], 0),
            (q_hbm, qg.at[0, 0], 1),
            (g_hbm, qg.at[0, 1], 1),
            (o_hbm, os_, 2),
            (l_hbm, ls, 3),
            (order_hbm, order, 4),
        )
    ]
    for load in loads:
        load.start()

    @pl.when(core == 0)
    def _():
        pltpu.make_async_copy(k_hbm, kv.at[0, 0], kv_recv.at[0, 0]).start()
        pltpu.make_async_copy(v_hbm, kv.at[0, 1], kv_recv.at[0, 1]).start()

    def remote(src, dst, send, recv, inner, head):
        return pltpu.make_async_remote_copy(
            src_ref=src,
            dst_ref=dst,
            send_sem=sem.at[send],
            recv_sem=recv,
            device_id={"inner": inner, "head": head},
            device_id_type=MESH,
        )

    def wait_bytes(ref, recv):
        remote(ref, ref, 0, recv, me, 1 - core).wait_recv()

    def wait_sent(ref, send):
        remote(ref, ref, send, pair_recv.at[0], me, 1 - core).wait_send()

    def slot_of(d):
        return d if d < m else n - 1 - d

    def kv_send(d):
        for i in range(2):
            place = (slot_of(d), i)
            remote(
                mine.at[i], kv.at[place], 0, kv_recv.at[place], chip(d), int(d >= m)
            ).start()

    wait_bytes(mine, sem.at[0])
    sent = jnp.where(
        me == 0,
        core,
        jnp.where(core == 1, n - split, split - 1),
    )
    pl.semaphore_wait(barrier, 1 + sent)

    pieces = [
        ((0, pl.ds(0, half)), entry.at[0]),
        ((0, pl.ds(half, half)), entry.at[1]),
        ((1,), entry.at[2]),
    ]

    @pl.when(me == 0)
    def _():
        @pl.when(core == 1)
        def _():
            for piece, ready in pieces:
                remote(mine.at[piece], kv.at[(m, *piece)], 0, ready, 1, 1).start()

    @pl.when(me != 0)
    def _():
        @pl.when(core == 1)
        def _():
            for d in reversed(range(split, n)):
                kv_send(d)

        @pl.when(core == 0)
        def _():
            @pl.when(me == 1)
            def _():
                pl.semaphore_signal(
                    entered, inc=1, device_id={"inner": me, "head": 1}, device_id_type=MESH
                )

            for d in range(1, m):
                kv_send(d)

    def middle_sends(when):
        @pl.when(jnp.logical_and(core == 0, when))
        def _():
            for d in range(m, split):
                kv_send(d)

    middle_sends(me > 1)

    wait_bytes(qg.at[0], sem.at[1])
    remote(qg.at[0], qg.at[1], 1, pair_recv.at[0], me, 1 - core).start()
    loads[4].wait()
    loads[5].wait()

    col = lax.broadcasted_iota(jnp.int32, (toks, rows), 1)
    spread = jnp.where(
        col // heads == lax.broadcasted_iota(jnp.int32, (toks, rows), 0), 1.0, 0.0
    )
    head_of = lax.broadcasted_iota(jnp.int32, (heads, rows), 1) % heads
    pick = head_of == lax.broadcasted_iota(jnp.int32, (heads, rows), 0)
    ones = jnp.ones((8, width), BF16)
    total = jnp.dot(
        ls[...], spread, preferred_element_type=F32, precision=lax.Precision.HIGHEST
    )
    total = jnp.sum(jnp.where(pick, total, 0.0), axis=0, keepdims=True)
    prod = os_[...].astype(F32) * qg[0, 1].astype(F32)
    high = prod.astype(BF16)
    rest = (prod - high.astype(F32)).astype(BF16)
    delta = dot(ones, high, NT) + dot(ones, rest, NT)
    stat[0, 0:1] = total * LOG2E
    stat[0, 1:2] = delta[0:1]
    remote(stat.at[0], stat.at[1], 2, pair_recv.at[1], me, 1 - core).start()

    loads[6].wait()

    relays = jnp.logical_and(me == 1, core == 1)

    @pl.when(relays)
    def _():
        def forward(piece, c):
            place = (slot_of(c), *piece)
            remote(
                kv.at[(m, *piece)], kv.at[place], 4, kv_recv.at[place[:2]], c, int(c >= m)
            ).start()

        pl.semaphore_wait(entered, 1)
        rest = [*range(m, n - 1), 1, *range(2, m)]
        for piece, ready in pieces[:2]:
            wait_bytes(kv.at[(m, *piece)], ready)
            forward(piece, n - 1)
        for c in rest:
            forward((0,), c)
        piece, ready = pieces[2]
        wait_bytes(kv.at[(m, *piece)], ready)
        for c in (*rest, n - 1):
            forward(piece, c)

    tok = (lax.broadcasted_iota(jnp.int32, (1, rows), 1)) // heads
    q_span = jnp.where(tok < half, order[2 * me], order[2 * me + 1])
    q_pos = q_span * half + tok % half
    q_span = jnp.concatenate([q_span, q_span], axis=1)
    q_pos = jnp.concatenate([q_pos, q_pos], axis=1)
    key_row = lax.broadcasted_iota(jnp.int32, (toks, 1), 0)

    with jax.named_scope("w_pair"):
        wait_bytes(qg.at[1], pair_recv.at[0])
        wait_bytes(stat.at[1], pair_recv.at[1])
    totals = jnp.concatenate([stat[0, 0:1], stat[1, 0:1]], axis=1)
    deltas = jnp.concatenate([stat[0, 1:2], stat[1, 1:2]], axis=1)

    def by_span(a, b):
        return jnp.where(key_row < half, a, b)

    def block(j):
        spans = [order[2 * owners[j] + h] for h in range(2)]
        queries = qg[:, 0].reshape(2 * rows, width)
        grads = qg[:, 1].reshape(2 * rows, width)
        with jax.named_scope(f"w_k{j}"):
            wait_bytes(kv.at[j, 0], kv_recv.at[j, 0])
        with jax.named_scope(f"dv{j}"):
            scores = dot(kv[j, 0], queries, NT)
            if j == 0:
                visible = by_span(*spans) * half + key_row % half <= q_pos
                probs = jnp.exp2(
                    jnp.where(visible, scores * (scale * LOG2E) - totals, -jnp.inf)
                )
            else:
                shifts = [jnp.where(k_span < q_span, totals, jnp.inf) for k_span in spans]
                probs = jnp.exp2(
                    jnp.concatenate(
                        [
                            scores[h * half : (h + 1) * half] * (scale * LOG2E) - shifts[h]
                            for h in range(2)
                        ]
                    )
                )
            yield 1, dot(probs.astype(BF16), grads)
        with jax.named_scope(f"w_v{j}"):
            wait_bytes(kv.at[j, 1], kv_recv.at[j, 1])
        with jax.named_scope(f"dk{j}"):
            grad_probs = dot(kv[j, 1], grads, NT)
            grad_scores = (probs * (grad_probs - deltas) * scale).astype(BF16)
            ds_all[j] = grad_scores
            yield 0, dot(grad_scores, queries)

    last = jnp.logical_and(core == 1, me == n - 1)
    held = jnp.logical_and(core == 0, me == n - 1)

    def grad_copy(j, i, head=1):
        spare = i == 0
        ready = grad_recv.at[jnp.where(last, 2, 0)] if spare else grad_recv.at[1]
        return remote(
            send_buf.at[j, i], recv_buf.at[i, me], 3 if head else 5, ready, owners[j], head
        )

    for j in range(m):
        for i, grad in block(j):
            send_buf[j, i] = grad.astype(BF16)
            if i == 0:
                pl.when(last)(lambda: grad_copy(j, i, 0).start())
            if j:
                pl.when(jnp.logical_not(held))(lambda: grad_copy(j, i).start())
            else:
                grad_copy(j, i).start()
            if (j, i) == (m - 1, 1):
                middle_sends(me == 1)

    def query_grad(i):
        total = None
        for j in range(m):
            term = dot(ds_all[j, :, i * rows : (i + 1) * rows], kv[j, 0], TN)
            total = term if total is None else total + term
        return total

    pl.when(relays)(lambda: wait_sent(recv_buf.at[:, 0 : n - 1], 4))

    with jax.named_scope("dq"):
        dq_send[...] = query_grad(1)
        dq_copy = remote(dq_send, dq_recv, 4, pair_recv.at[2], me, 1 - core)
        dq_copy.start()
        own_grad = query_grad(0)

    @pl.when(held)
    def _():
        for j in range(1, m):
            for i in (1, 0):
                grad_copy(j, i).start()

    lower = me < m

    def sum_near(count):
        with jax.named_scope("w_near"):
            wait_bytes(recv_buf.at[0, 0:count], grad_recv.at[0])
        return sum(recv_buf[0, c].astype(F32) for c in range(count))

    wait_sent(stat.at[0], 2)

    @pl.when(jnp.logical_and(core == 1, lower))
    def _():
        part[...] = sum_near(n - 1)
        remote(part, part, 2, pair_recv.at[4], me, 0).start()

    with jax.named_scope("w_dq"):
        dq_copy.wait_recv()
    dq_ref[...] = (own_grad + dq_recv[...]).astype(BF16)

    with jax.named_scope("w_sends"):
        wait_sent(qg.at[0], 1)
        wait_sent(send_buf, 3)
        dq_copy.wait_send()

        @pl.when(core == 1)
        def _():
            pl.when(me == 0)(lambda: wait_sent(mine, 0))
            pl.when(me != 0)(lambda: wait_sent(recv_buf.at[:, 0 : n - split], 0))

        @pl.when(jnp.logical_and(core == 0, me != 0))
        def _():
            wait_sent(recv_buf.at[:, 1:split], 0)

    def sum_far():
        with jax.named_scope("w_far"):
            wait_bytes(recv_buf.at[0, n - 1], grad_recv.at[2])
        kv_ref[0] = (part[...] + recv_buf[0, n - 1].astype(F32)).astype(BF16)

    @pl.when(core == 1)
    def _():
        pl.when(last)(lambda: wait_sent(recv_buf.at[0, 0:m], 5))
        with jax.named_scope("w_v"):
            wait_bytes(recv_buf.at[1], grad_recv.at[1])
        kv_ref[1] = sum(recv_buf[1, c].astype(F32) for c in range(n)).astype(BF16)
        remote(kv_ref.at[1], kv_ref.at[1], 5, pair_recv.at[3], me, 0).start()

        @pl.when(jnp.logical_not(lower))
        def _():
            kv_ref[0] = sum_near(n).astype(BF16)
            remote(kv_ref.at[0], kv_ref.at[0], 5, pair_recv.at[3], me, 0).start()
            wait_sent(kv_ref, 5)

        @pl.when(lower)
        def _():
            sum_far()
            with jax.named_scope("w_finsend"):
                wait_sent(kv_ref.at[1], 5)
                wait_sent(part, 2)

    @pl.when(core == 0)
    def _():
        @pl.when(jnp.logical_not(lower))
        def _():
            with jax.named_scope("w_fin"):
                wait_bytes(kv_ref, pair_recv.at[3])

        @pl.when(lower)
        def _():
            with jax.named_scope("w_part"):
                wait_bytes(part, pair_recv.at[4])
            sum_far()
            with jax.named_scope("w_finv"):
                wait_bytes(kv_ref.at[1], pair_recv.at[3])


def store_kernel(dq_ref, kv_ref, dq_hbm, dk_hbm, dv_hbm, sem):
    pairs = ((dq_ref, dq_hbm), (kv_ref.at[0], dk_hbm), (kv_ref.at[1], dv_hbm))
    copies = [pltpu.make_async_copy(a, b, sem.at[i]) for i, (a, b) in enumerate(pairs)]
    for copy in copies:
        copy.start()
    for copy in copies:
        copy.wait()


def body(n, queries, keys, values, out, log_total, d_out, span_order):
    _, toks, heads, width = queries.shape
    rows = toks * heads
    m = n // 2
    flat = lambda x: x.reshape(rows, width)
    anywhere = pl.BlockSpec(memory_space=pltpu.HBM)
    in_vmem = pl.BlockSpec(memory_space=pltpu.VMEM)
    dq, dkv = pl.pallas_call(
        functools.partial(kernel, n, heads),
        out_shape=(
            pltpu.VMEM((rows, width), BF16),
            pltpu.VMEM((2, toks, width), BF16),
        ),
        in_specs=[anywhere] * 7,
        out_specs=(in_vmem,) * 2,
        scratch_shapes=[
            pltpu.VMEM((2, 2, rows, width), BF16),
            pltpu.VMEM((rows, width), BF16),
            pltpu.VMEM((heads, toks), F32),
            pltpu.VMEM((2, toks, width), BF16),
            pltpu.VMEM((m + 1, 2, toks, width), BF16),
            pltpu.VMEM((2, 8, rows), F32),
            pltpu.VMEM((m, toks, 2 * rows), BF16),
            pltpu.VMEM((m, 2, toks, width), BF16),
            pltpu.VMEM((2, n, toks, width), BF16),
            pltpu.VMEM((toks, width), F32),
            pltpu.VMEM((rows, width), F32),
            pltpu.VMEM((rows, width), F32),
            pltpu.SMEM((span_order.shape[1],), jnp.int32),
            pltpu.SemaphoreType.DMA((6,)),
            pltpu.SemaphoreType.DMA((5,)),
            pltpu.SemaphoreType.DMA((m, 2)),
            pltpu.SemaphoreType.DMA((3,)),
            pltpu.SemaphoreType.DMA((3,)),
            pltpu.SemaphoreType.REGULAR,
        ],
        compiler_params=pltpu.CompilerParams(collective_id=0, has_side_effects=True),
    )(
        flat(queries),
        keys[0],
        values[0],
        flat(out),
        log_total[0],
        flat(d_out),
        span_order[0],
    )
    dq, dk, dv = pl.pallas_call(
        store_kernel,
        out_shape=(
            jax.ShapeDtypeStruct((rows, width), BF16),
            jax.ShapeDtypeStruct((toks, width), BF16),
            jax.ShapeDtypeStruct((toks, width), BF16),
        ),
        in_specs=[in_vmem] * 2,
        out_specs=(anywhere,) * 3,
        scratch_shapes=[pltpu.SemaphoreType.DMA((3,))],
        compiler_params=pltpu.CompilerParams(vmem_limit_bytes=2**20),
    )(dq, dkv)
    return dq.reshape(queries.shape), dk[None], dv[None]


def solution(mesh):
    seq = ("groups", "outer")
    wide = P(seq, "inner", "head", None)
    narrow = P(seq, "inner", None)
    return jax.shard_map(
        functools.partial(body, mesh.shape["inner"]),
        mesh=mesh,
        in_specs=(wide, narrow, narrow, wide, P(seq, "head", "inner"), wide, P(seq, None)),
        out_specs=(wide, narrow, narrow),
        check_vma=False,
    )
```

```python
import functools
import math

import jax
import jax.numpy as jnp
from jax import lax
from jax.experimental import pallas as pl
from jax.experimental.pallas import tpu as pltpu
from jax.sharding import PartitionSpec as P

MESH = pl.DeviceIdType.MESH
F32 = jnp.float32
BF16 = jnp.bfloat16
NT = (((1,), (1,)), ((), ()))
TN = (((0,), (0,)), ((), ()))
LOG2E = math.log2(math.e)


def dot(a, b, dims=(((1,), (0,)), ((), ()))):
    return lax.dot_general(a, b, dims, preferred_element_type=F32)


def kernel(
    n,
    heads,
    q_hbm,
    k_hbm,
    v_hbm,
    o_hbm,
    l_hbm,
    g_hbm,
    order_hbm,
    out_ref,
    qg,
    os_,
    ls,
    mine,
    kv,
    stat,
    ds_all,
    send_buf,
    recv_buf,
    part,
    dq_send,
    dq_recv,
    order,
    sem,
    pair_recv,
    kv_recv,
    grad_recv,
    entry,
    entered,
):
    me = lax.axis_index("inner")
    core = lax.axis_index("head")
    m = n // 2
    split = m + m // 2
    toks, width = kv.shape[2], kv.shape[3]
    half = toks // 2
    rows = qg.shape[2]
    dq_ref, kv_out = out_ref.at[pl.ds(0, rows)], out_ref.at[pl.ds(rows, 2 * toks)]
    grad_out = [out_ref.at[pl.ds(rows + i * toks, toks)] for i in range(2)]
    scale = 1.0 / math.sqrt(width)
    partner = {"head": 1 - core}

    def chip(d):
        at = me
        for k in range(n.bit_length()):
            if d >> k & 1:
                at = at + (1 - 2 * ((me // 2**k) % 2)) * 2**k
        return at

    owners = [chip(j) + core * (chip(n - 1 - j) - chip(j)) for j in range(m)]

    barrier = pltpu.get_barrier_semaphore()

    def greet(inner, head, when=None):
        def signal():
            pl.semaphore_signal(
                barrier, inc=1, device_id={"inner": inner, "head": head}, device_id_type=MESH
            )

        signal() if when is None else pl.when(when)(signal)

    @pl.when(core == 1)
    def _():
        greet(0, 1, me == 1)
        for d in reversed(range(split, n)):
            greet(chip(d), 1, chip(d) != 0)
        for d in reversed(range(m, split)):
            greet(chip(d), 0, chip(d) != 0)
        greet(me, 0)

    @pl.when(core == 0)
    def _():
        for d in range(1, m):
            greet(chip(d), 0, chip(d) != 0)
        greet(me, 1)

    loads = [
        pltpu.make_async_copy(src, dst, sem.at[i])
        for src, dst, i in (
            (k_hbm, mine.at[0], 0),
            (v_hbm, mine.at[1], 0),
            (q_hbm, qg.at[0, 0], 1),
            (g_hbm, qg.at[0, 1], 1),
            (o_hbm, os_, 2),
            (l_hbm, ls, 3),
            (order_hbm, order, 4),
        )
    ]
    for load in loads:
        load.start()

    @pl.when(core == 0)
    def _():
        pltpu.make_async_copy(k_hbm, kv.at[0, 0], kv_recv.at[0, 0]).start()
        pltpu.make_async_copy(v_hbm, kv.at[0, 1], kv_recv.at[0, 1]).start()

    def remote(src, dst, send, recv, inner, head):
        return pltpu.make_async_remote_copy(
            src_ref=src,
            dst_ref=dst,
            send_sem=sem.at[send],
            recv_sem=recv,
            device_id={"inner": inner, "head": head},
            device_id_type=MESH,
        )

    def wait_bytes(ref, recv):
        remote(ref, ref, 0, recv, me, 1 - core).wait_recv()

    def wait_sent(ref, send):
        remote(ref, ref, send, pair_recv.at[0], me, 1 - core).wait_send()

    def slot_of(d):
        return d if d < m else n - 1 - d

    def kv_send(d):
        for i in range(2):
            place = (slot_of(d), i)
            remote(
                mine.at[i], kv.at[place], 0, kv_recv.at[place], chip(d), int(d >= m)
            ).start()

    wait_bytes(mine, sem.at[0])
    sent = jnp.where(
        me == 0,
        core,
        jnp.where(core == 1, n - split, split - 1),
    )
    pl.semaphore_wait(barrier, 1 + sent)

    pieces = [
        ((0, pl.ds(0, half)), entry.at[0]),
        ((0, pl.ds(half, half)), entry.at[1]),
        ((1,), entry.at[2]),
    ]

    @pl.when(me == 0)
    def _():
        @pl.when(core == 1)
        def _():
            for piece, ready in pieces:
                remote(mine.at[piece], kv.at[(m, *piece)], 0, ready, 1, 1).start()

    @pl.when(me != 0)
    def _():
        @pl.when(core == 1)
        def _():
            for d in reversed(range(split, n)):
                kv_send(d)

        @pl.when(core == 0)
        def _():
            @pl.when(me == 1)
            def _():
                pl.semaphore_signal(
                    entered, inc=1, device_id={"inner": me, "head": 1}, device_id_type=MESH
                )

            @pl.when(me == 1)
            def _():
                for d in range(1, m):
                    kv_send(d)

    def middle_sends(when):
        @pl.when(jnp.logical_and(core == 0, when))
        def _():
            for d in range(m, split):
                kv_send(d)

    middle_sends(me > 1)

    @pl.when(jnp.logical_and(core == 0, me > 1))
    def _():
        for d in range(1, m):
            kv_send(d)

    wait_bytes(qg.at[0], sem.at[1])
    remote(qg.at[0], qg.at[1], 1, pair_recv.at[0], me, 1 - core).start()
    loads[4].wait()
    loads[5].wait()

    col = lax.broadcasted_iota(jnp.int32, (toks, rows), 1)
    spread = jnp.where(
        col // heads == lax.broadcasted_iota(jnp.int32, (toks, rows), 0), 1.0, 0.0
    )
    head_of = lax.broadcasted_iota(jnp.int32, (heads, rows), 1) % heads
    pick = head_of == lax.broadcasted_iota(jnp.int32, (heads, rows), 0)
    ones = jnp.ones((8, width), BF16)
    total = jnp.dot(
        ls[...], spread, preferred_element_type=F32, precision=lax.Precision.HIGHEST
    )
    total = jnp.sum(jnp.where(pick, total, 0.0), axis=0, keepdims=True)
    prod = os_[...].astype(F32) * qg[0, 1].astype(F32)
    high = prod.astype(BF16)
    rest = (prod - high.astype(F32)).astype(BF16)
    delta = dot(ones, high, NT) + dot(ones, rest, NT)
    stat[0, 0:1] = total * LOG2E
    stat[0, 1:2] = delta[0:1]
    remote(stat.at[0], stat.at[1], 2, pair_recv.at[1], me, 1 - core).start()

    loads[6].wait()

    relays = jnp.logical_and(me == 1, core == 1)

    @pl.when(relays)
    def _():
        def forward(piece, c):
            place = (slot_of(c), *piece)
            remote(
                kv.at[(m, *piece)], kv.at[place], 4, kv_recv.at[place[:2]], c, int(c >= m)
            ).start()

        pl.semaphore_wait(entered, 1)
        rest = [*range(m, n - 1), 1, *range(2, m)]
        for piece, ready in pieces[:2]:
            wait_bytes(kv.at[(m, *piece)], ready)
            forward(piece, n - 1)
        for c in rest:
            forward((0,), c)
        piece, ready = pieces[2]
        wait_bytes(kv.at[(m, *piece)], ready)
        for c in (*rest, n - 1):
            forward(piece, c)

    tok = (lax.broadcasted_iota(jnp.int32, (1, rows), 1)) // heads
    q_span = jnp.where(tok < half, order[2 * me], order[2 * me + 1])
    q_pos = q_span * half + tok % half
    q_span = jnp.concatenate([q_span, q_span], axis=1)
    q_pos = jnp.concatenate([q_pos, q_pos], axis=1)
    key_row = lax.broadcasted_iota(jnp.int32, (toks, 1), 0)

    with jax.named_scope("w_pair"):
        wait_bytes(qg.at[1], pair_recv.at[0])
        wait_bytes(stat.at[1], pair_recv.at[1])
    totals = jnp.concatenate([stat[0, 0:1], stat[1, 0:1]], axis=1)
    deltas = jnp.concatenate([stat[0, 1:2], stat[1, 1:2]], axis=1)

    def by_span(a, b):
        return jnp.where(key_row < half, a, b)

    def block(j):
        spans = [order[2 * owners[j] + h] for h in range(2)]
        queries = qg[:, 0].reshape(2 * rows, width)
        grads = qg[:, 1].reshape(2 * rows, width)
        with jax.named_scope(f"w_k{j}"):
            wait_bytes(kv.at[j, 0], kv_recv.at[j, 0])
        with jax.named_scope(f"dv{j}"):
            scores = dot(kv[j, 0], queries, NT)
            if j == 0:
                visible = by_span(*spans) * half + key_row % half <= q_pos
                probs = jnp.exp2(
                    jnp.where(visible, scores * (scale * LOG2E) - totals, -jnp.inf)
                )
            else:
                shifts = [jnp.where(k_span < q_span, totals, jnp.inf) for k_span in spans]
                probs = jnp.exp2(
                    jnp.concatenate(
                        [
                            scores[h * half : (h + 1) * half] * (scale * LOG2E) - shifts[h]
                            for h in range(2)
                        ]
                    )
                )
            yield 1, dot(probs.astype(BF16), grads)
        with jax.named_scope(f"w_v{j}"):
            wait_bytes(kv.at[j, 1], kv_recv.at[j, 1])
        with jax.named_scope(f"dk{j}"):
            grad_probs = dot(kv[j, 1], grads, NT)
            grad_scores = (probs * (grad_probs - deltas) * scale).astype(BF16)
            ds_all[j] = grad_scores
            yield 0, dot(grad_scores, queries)

    last = jnp.logical_and(core == 1, me == n - 1)
    held = jnp.logical_and(core == 0, me == n - 1)

    def grad_copy(j, i, head=1):
        spare = i == 0
        ready = grad_recv.at[jnp.where(last, 2, 0)] if spare else grad_recv.at[1]
        return remote(
            send_buf.at[j, i], recv_buf.at[i, me], 3 if head else 5, ready, owners[j], head
        )

    for j in range(m):
        for i, grad in block(j):
            send_buf[j, i] = grad.astype(BF16)
            if i == 0:
                pl.when(last)(lambda: grad_copy(j, i, 0).start())
            if j:
                pl.when(jnp.logical_not(held))(lambda: grad_copy(j, i).start())
            else:
                grad_copy(j, i).start()
            if (j, i) == (m - 1, 1):
                middle_sends(me == 1)

    def query_grad(i):
        total = None
        for j in range(m):
            term = dot(ds_all[j, :, i * rows : (i + 1) * rows], kv[j, 0], TN)
            total = term if total is None else total + term
        return total

    pl.when(relays)(lambda: wait_sent(recv_buf.at[:, 0 : n - 1], 4))

    with jax.named_scope("dq"):
        dq_send[...] = query_grad(1)
        dq_copy = remote(dq_send, dq_recv, 4, pair_recv.at[2], me, 1 - core)
        dq_copy.start()
        own_grad = query_grad(0)

    @pl.when(held)
    def _():
        for j in range(1, m):
            for i in (1, 0):
                grad_copy(j, i).start()

    lower = me < m

    def sum_near(count):
        with jax.named_scope("w_near"):
            wait_bytes(recv_buf.at[0, 0:count], grad_recv.at[0])
        return sum(recv_buf[0, c].astype(F32) for c in range(count))

    wait_sent(stat.at[0], 2)

    def finish_values():
        with jax.named_scope("w_v"):
            wait_bytes(recv_buf.at[1], grad_recv.at[1])
        grad_out[1][...] = sum(recv_buf[1, c].astype(F32) for c in range(n)).astype(BF16)
        remote(grad_out[1], grad_out[1], 5, pair_recv.at[3], me, 0).start()

    pl.when(jnp.logical_and(core == 1, me == 0))(finish_values)

    @pl.when(jnp.logical_and(core == 1, lower))
    def _():
        part[...] = sum_near(n - 1)
        remote(part, part, 2, pair_recv.at[4], me, 0).start()

    with jax.named_scope("w_dq"):
        dq_copy.wait_recv()
    dq_ref[...] = (own_grad + dq_recv[...]).astype(BF16)

    with jax.named_scope("w_sends"):
        wait_sent(qg.at[0], 1)
        wait_sent(send_buf, 3)
        dq_copy.wait_send()

        @pl.when(core == 1)
        def _():
            pl.when(me == 0)(lambda: wait_sent(mine, 0))
            pl.when(me != 0)(lambda: wait_sent(recv_buf.at[:, 0 : n - split], 0))

        @pl.when(jnp.logical_and(core == 0, me != 0))
        def _():
            wait_sent(recv_buf.at[:, 1:split], 0)

    def sum_far():
        with jax.named_scope("w_far"):
            wait_bytes(recv_buf.at[0, n - 1], grad_recv.at[2])
        grad_out[0][...] = (part[...] + recv_buf[0, n - 1].astype(F32)).astype(BF16)

    @pl.when(core == 1)
    def _():
        pl.when(last)(lambda: wait_sent(recv_buf.at[0, 0:m], 5))
        pl.when(me != 0)(finish_values)

        @pl.when(jnp.logical_not(lower))
        def _():
            grad_out[0][...] = sum_near(n).astype(BF16)
            remote(grad_out[0], grad_out[0], 5, pair_recv.at[3], me, 0).start()
            wait_sent(kv_out, 5)

        @pl.when(lower)
        def _():
            sum_far()
            with jax.named_scope("w_finsend"):
                wait_sent(grad_out[1], 5)
                wait_sent(part, 2)

    @pl.when(core == 0)
    def _():
        @pl.when(jnp.logical_not(lower))
        def _():
            with jax.named_scope("w_fin"):
                wait_bytes(kv_out, pair_recv.at[3])

        @pl.when(lower)
        def _():
            with jax.named_scope("w_part"):
                wait_bytes(part, pair_recv.at[4])
            sum_far()
            with jax.named_scope("w_finv"):
                wait_bytes(grad_out[1], pair_recv.at[3])


def store_kernel(out_ref, dq_hbm, dk_hbm, dv_hbm, sem):
    start = 0
    for dst in (dq_hbm, dk_hbm, dv_hbm):
        span = pl.ds(start, dst.shape[0])
        pltpu.make_async_copy(out_ref.at[span], dst, sem).start()
        start += dst.shape[0]
    pltpu.make_async_copy(out_ref, out_ref, sem).wait()


def body(n, queries, keys, values, out, log_total, d_out, span_order):
    _, toks, heads, width = queries.shape
    rows = toks * heads
    m = n // 2
    flat = lambda x: x.reshape(rows, width)
    anywhere = pl.BlockSpec(memory_space=pltpu.HBM)
    in_vmem = pl.BlockSpec(memory_space=pltpu.VMEM)
    grads = pl.pallas_call(
        functools.partial(kernel, n, heads),
        out_shape=pltpu.VMEM((rows + 2 * toks, width), BF16),
        in_specs=[anywhere] * 7,
        out_specs=in_vmem,
        scratch_shapes=[
            pltpu.VMEM((2, 2, rows, width), BF16),
            pltpu.VMEM((rows, width), BF16),
            pltpu.VMEM((heads, toks), F32),
            pltpu.VMEM((2, toks, width), BF16),
            pltpu.VMEM((m + 1, 2, toks, width), BF16),
            pltpu.VMEM((2, 8, rows), F32),
            pltpu.VMEM((m, toks, 2 * rows), BF16),
            pltpu.VMEM((m, 2, toks, width), BF16),
            pltpu.VMEM((2, n, toks, width), BF16),
            pltpu.VMEM((toks, width), F32),
            pltpu.VMEM((rows, width), F32),
            pltpu.VMEM((rows, width), F32),
            pltpu.SMEM((span_order.shape[1],), jnp.int32),
            pltpu.SemaphoreType.DMA((6,)),
            pltpu.SemaphoreType.DMA((5,)),
            pltpu.SemaphoreType.DMA((m, 2)),
            pltpu.SemaphoreType.DMA((3,)),
            pltpu.SemaphoreType.DMA((3,)),
            pltpu.SemaphoreType.REGULAR,
        ],
        compiler_params=pltpu.CompilerParams(collective_id=0, has_side_effects=True),
    )(
        flat(queries),
        keys[0],
        values[0],
        flat(out),
        log_total[0],
        flat(d_out),
        span_order[0],
    )
    dq, dk, dv = pl.pallas_call(
        store_kernel,
        out_shape=(
            jax.ShapeDtypeStruct((rows, width), BF16),
            jax.ShapeDtypeStruct((toks, width), BF16),
            jax.ShapeDtypeStruct((toks, width), BF16),
        ),
        in_specs=[in_vmem],
        out_specs=(anywhere,) * 3,
        scratch_shapes=[pltpu.SemaphoreType.DMA],
        compiler_params=pltpu.CompilerParams(vmem_limit_bytes=2**20),
    )(grads)
    return dq.reshape(queries.shape), dk[None], dv[None]


def solution(mesh):
    seq = ("groups", "outer")
    wide = P(seq, "inner", "head", None)
    narrow = P(seq, "inner", None)
    return jax.shard_map(
        functools.partial(body, mesh.shape["inner"]),
        mesh=mesh,
        in_specs=(wide, narrow, narrow, wide, P(seq, "head", "inner"), wide, P(seq, None)),
        out_specs=(wide, narrow, narrow),
        check_vma=False,
    )
```

```python
import functools
import math

import jax
import jax.numpy as jnp
from jax import lax
from jax.experimental import pallas as pl
from jax.experimental.pallas import tpu as pltpu
from jax.sharding import PartitionSpec as P

MESH = pl.DeviceIdType.MESH
F32 = jnp.float32
BF16 = jnp.bfloat16
NT = (((1,), (1,)), ((), ()))
TN = (((0,), (0,)), ((), ()))
LOG2E = math.log2(math.e)


def dot(a, b, dims=(((1,), (0,)), ((), ()))):
    return lax.dot_general(a, b, dims, preferred_element_type=F32)


def kernel(
    n,
    heads,
    q_hbm,
    k_hbm,
    v_hbm,
    o_hbm,
    l_hbm,
    g_hbm,
    order_hbm,
    out_ref,
    qg,
    os_,
    ls,
    mine,
    kv,
    stat,
    ds_all,
    send_buf,
    recv_buf,
    part,
    dq_send,
    dq_recv,
    order,
    sem,
    pair_recv,
    kv_recv,
    grad_recv,
    entry,
    entered,
):
    me = lax.axis_index("inner")
    core = lax.axis_index("head")
    m = n // 2
    split = m + m // 2
    toks, width = kv.shape[2], kv.shape[3]
    half = toks // 2
    rows = qg.shape[2]
    dq_ref, kv_out = out_ref.at[pl.ds(0, rows)], out_ref.at[pl.ds(rows, 2 * toks)]
    grad_out = [out_ref.at[pl.ds(rows + i * toks, toks)] for i in range(2)]
    scale = 1.0 / math.sqrt(width)
    partner = {"head": 1 - core}

    def chip(d):
        at = me
        for k in range(n.bit_length()):
            if d >> k & 1:
                at = at + (1 - 2 * ((me // 2**k) % 2)) * 2**k
        return at

    owners = [chip(j) + core * (chip(n - 1 - j) - chip(j)) for j in range(m)]

    barrier = pltpu.get_barrier_semaphore()

    def greet(inner, head, when=None):
        def signal():
            pl.semaphore_signal(
                barrier, inc=1, device_id={"inner": inner, "head": head}, device_id_type=MESH
            )

        signal() if when is None else pl.when(when)(signal)

    @pl.when(core == 1)
    def _():
        greet(0, 1, me == 1)
        for d in reversed(range(split, n)):
            greet(chip(d), 1, chip(d) != 0)
        for d in reversed(range(m, split)):
            greet(chip(d), 0, chip(d) != 0)
        greet(me, 0)

    @pl.when(core == 0)
    def _():
        for d in range(1, m):
            greet(chip(d), 0, chip(d) != 0)
        greet(me, 1)

    loads = [
        pltpu.make_async_copy(src, dst, sem.at[i])
        for src, dst, i in (
            (k_hbm, mine.at[0], 0),
            (v_hbm, mine.at[1], 0),
            (q_hbm, qg.at[0, 0], 1),
            (g_hbm, qg.at[0, 1], 1),
            (o_hbm, os_, 2),
            (l_hbm, ls, 3),
            (order_hbm, order, 4),
        )
    ]
    for load in loads:
        load.start()

    @pl.when(core == 0)
    def _():
        pltpu.make_async_copy(k_hbm, kv.at[0, 0], kv_recv.at[0, 0]).start()
        pltpu.make_async_copy(v_hbm, kv.at[0, 1], kv_recv.at[0, 1]).start()

    def remote(src, dst, send, recv, inner, head):
        return pltpu.make_async_remote_copy(
            src_ref=src,
            dst_ref=dst,
            send_sem=sem.at[send],
            recv_sem=recv,
            device_id={"inner": inner, "head": head},
            device_id_type=MESH,
        )

    def wait_bytes(ref, recv):
        remote(ref, ref, 0, recv, me, 1 - core).wait_recv()

    def wait_sent(ref, send):
        remote(ref, ref, send, pair_recv.at[0], me, 1 - core).wait_send()

    def slot_of(d):
        return d if d < m else n - 1 - d

    def kv_send(d):
        for i in range(2):
            place = (slot_of(d), i)
            remote(
                mine.at[i], kv.at[place], 0, kv_recv.at[place], chip(d), int(d >= m)
            ).start()

    wait_bytes(mine, sem.at[0])
    sent = jnp.where(
        me == 0,
        core,
        jnp.where(core == 1, n - split, split - 1),
    )
    pl.semaphore_wait(barrier, 1 + sent)

    pieces = [
        ((0, pl.ds(0, half)), entry.at[0]),
        ((0, pl.ds(half, half)), entry.at[1]),
        ((1,), entry.at[2]),
    ]

    @pl.when(me == 0)
    def _():
        @pl.when(core == 1)
        def _():
            for piece, ready in pieces:
                remote(mine.at[piece], kv.at[(m, *piece)], 0, ready, 1, 1).start()

    @pl.when(me != 0)
    def _():
        @pl.when(core == 1)
        def _():
            for d in reversed(range(split, n)):
                kv_send(d)

        @pl.when(core == 0)
        def _():
            @pl.when(me == 1)
            def _():
                pl.semaphore_signal(
                    entered, inc=1, device_id={"inner": me, "head": 1}, device_id_type=MESH
                )

            @pl.when(me == 1)
            def _():
                for d in range(1, m):
                    kv_send(d)

    def middle_sends(when):
        @pl.when(jnp.logical_and(core == 0, when))
        def _():
            for d in range(m, split):
                kv_send(d)

    middle_sends(me > 1)

    @pl.when(jnp.logical_and(core == 0, me > 1))
    def _():
        for d in range(1, m):
            kv_send(d)

    wait_bytes(qg.at[0], sem.at[1])
    remote(qg.at[0], qg.at[1], 1, pair_recv.at[0], me, 1 - core).start()
    loads[4].wait()
    loads[5].wait()

    col = lax.broadcasted_iota(jnp.int32, (toks, rows), 1)
    spread = jnp.where(
        col // heads == lax.broadcasted_iota(jnp.int32, (toks, rows), 0), 1.0, 0.0
    )
    head_of = lax.broadcasted_iota(jnp.int32, (heads, rows), 1) % heads
    pick = head_of == lax.broadcasted_iota(jnp.int32, (heads, rows), 0)
    ones = jnp.ones((8, width), BF16)
    total = jnp.dot(
        ls[...], spread, preferred_element_type=F32, precision=lax.Precision.HIGHEST
    )
    total = jnp.sum(jnp.where(pick, total, 0.0), axis=0, keepdims=True)
    prod = os_[...].astype(F32) * qg[0, 1].astype(F32)
    high = prod.astype(BF16)
    rest = (prod - high.astype(F32)).astype(BF16)
    delta = dot(ones, high, NT) + dot(ones, rest, NT)
    stat[0, 0:1] = total * LOG2E
    stat[0, 1:2] = delta[0:1]
    remote(stat.at[0], stat.at[1], 2, pair_recv.at[1], me, 1 - core).start()

    loads[6].wait()

    relays = jnp.logical_and(me == 1, core == 1)

    @pl.when(relays)
    def _():
        def forward(piece, c):
            place = (slot_of(c), *piece)
            remote(
                kv.at[(m, *piece)], kv.at[place], 4, kv_recv.at[place[:2]], c, int(c >= m)
            ).start()

        greeted = [c for c in range(m, n - 1) if c ^ 1 >= split]
        rest = [c for c in range(1, n - 1) if c not in greeted]
        for piece, ready in pieces[:2]:
            wait_bytes(kv.at[(m, *piece)], ready)
            for c in greeted:
                forward(piece, c)
        pl.semaphore_wait(entered, 1)
        for c in (n - 1, *rest):
            forward((0,), c)
        piece, ready = pieces[2]
        wait_bytes(kv.at[(m, *piece)], ready)
        for c in (*greeted, *rest, n - 1):
            forward(piece, c)

    tok = (lax.broadcasted_iota(jnp.int32, (1, rows), 1)) // heads
    q_span = jnp.where(tok < half, order[2 * me], order[2 * me + 1])
    q_pos = q_span * half + tok % half
    q_span = jnp.concatenate([q_span, q_span], axis=1)
    q_pos = jnp.concatenate([q_pos, q_pos], axis=1)
    key_row = lax.broadcasted_iota(jnp.int32, (toks, 1), 0)

    with jax.named_scope("w_pair"):
        wait_bytes(qg.at[1], pair_recv.at[0])
        wait_bytes(stat.at[1], pair_recv.at[1])
    totals = jnp.concatenate([stat[0, 0:1], stat[1, 0:1]], axis=1)
    deltas = jnp.concatenate([stat[0, 1:2], stat[1, 1:2]], axis=1)

    def by_span(a, b):
        return jnp.where(key_row < half, a, b)

    def block(j):
        spans = [order[2 * owners[j] + h] for h in range(2)]
        queries = qg[:, 0].reshape(2 * rows, width)
        grads = qg[:, 1].reshape(2 * rows, width)
        with jax.named_scope(f"w_k{j}"):
            wait_bytes(kv.at[j, 0], kv_recv.at[j, 0])
        with jax.named_scope(f"dv{j}"):
            scores = dot(kv[j, 0], queries, NT)
            if j == 0:
                visible = by_span(*spans) * half + key_row % half <= q_pos
                probs = jnp.exp2(
                    jnp.where(visible, scores * (scale * LOG2E) - totals, -jnp.inf)
                )
            else:
                shifts = [jnp.where(k_span < q_span, totals, jnp.inf) for k_span in spans]
                probs = jnp.exp2(
                    jnp.concatenate(
                        [
                            scores[h * half : (h + 1) * half] * (scale * LOG2E) - shifts[h]
                            for h in range(2)
                        ]
                    )
                )
            yield 1, dot(probs.astype(BF16), grads)
        with jax.named_scope(f"w_v{j}"):
            wait_bytes(kv.at[j, 1], kv_recv.at[j, 1])
        with jax.named_scope(f"dk{j}"):
            grad_probs = dot(kv[j, 1], grads, NT)
            grad_scores = (probs * (grad_probs - deltas) * scale).astype(BF16)
            ds_all[j] = grad_scores
            yield 0, dot(grad_scores, queries)

    last = jnp.logical_and(core == 1, me == n - 1)
    held = jnp.logical_and(core == 0, me == n - 1)

    def grad_copy(j, i, head=1):
        spare = i == 0
        ready = grad_recv.at[jnp.where(last, 2, 0)] if spare else grad_recv.at[1]
        return remote(
            send_buf.at[j, i], recv_buf.at[i, me], 3 if head else 5, ready, owners[j], head
        )

    for j in range(m):
        for i, grad in block(j):
            send_buf[j, i] = grad.astype(BF16)
            if i == 0:
                pl.when(last)(lambda: grad_copy(j, i, 0).start())
            if j:
                pl.when(jnp.logical_not(held))(lambda: grad_copy(j, i).start())
            else:
                grad_copy(j, i).start()
            if (j, i) == (m - 1, 1):
                middle_sends(me == 1)

    def query_grad(i):
        total = None
        for j in range(m):
            term = dot(ds_all[j, :, i * rows : (i + 1) * rows], kv[j, 0], TN)
            total = term if total is None else total + term
        return total

    pl.when(relays)(lambda: wait_sent(recv_buf.at[:, 0 : n - 1], 4))

    with jax.named_scope("dq"):
        dq_send[...] = query_grad(1)
        dq_copy = remote(dq_send, dq_recv, 4, pair_recv.at[2], me, 1 - core)
        dq_copy.start()
        own_grad = query_grad(0)

    @pl.when(held)
    def _():
        for j in range(1, m):
            for i in (1, 0):
                grad_copy(j, i).start()

    lower = me < m

    def sum_near(count):
        with jax.named_scope("w_near"):
            wait_bytes(recv_buf.at[0, 0:count], grad_recv.at[0])
        return sum(recv_buf[0, c].astype(F32) for c in range(count))

    wait_sent(stat.at[0], 2)

    def finish_values():
        with jax.named_scope("w_v"):
            wait_bytes(recv_buf.at[1], grad_recv.at[1])
        grad_out[1][...] = sum(recv_buf[1, c].astype(F32) for c in range(n)).astype(BF16)
        remote(grad_out[1], grad_out[1], 5, pair_recv.at[3], me, 0).start()

    @pl.when(jnp.logical_and(core == 1, lower))
    def _():
        part[...] = sum_near(n - 1)
        remote(part, part, 2, pair_recv.at[4], me, 0).start()

    pl.when(jnp.logical_and(core == 1, me == 0))(finish_values)

    with jax.named_scope("w_dq"):
        dq_copy.wait_recv()
    dq_ref[...] = (own_grad + dq_recv[...]).astype(BF16)

    with jax.named_scope("w_sends"):
        wait_sent(qg.at[0], 1)
        wait_sent(send_buf, 3)
        dq_copy.wait_send()

        @pl.when(core == 1)
        def _():
            pl.when(me == 0)(lambda: wait_sent(mine, 0))
            pl.when(me != 0)(lambda: wait_sent(recv_buf.at[:, 0 : n - split], 0))

        @pl.when(jnp.logical_and(core == 0, me != 0))
        def _():
            wait_sent(recv_buf.at[:, 1:split], 0)

    def sum_far():
        with jax.named_scope("w_far"):
            wait_bytes(recv_buf.at[0, n - 1], grad_recv.at[2])
        grad_out[0][...] = (part[...] + recv_buf[0, n - 1].astype(F32)).astype(BF16)

    @pl.when(core == 1)
    def _():
        pl.when(last)(lambda: wait_sent(recv_buf.at[0, 0:m], 5))
        pl.when(me != 0)(finish_values)

        @pl.when(jnp.logical_not(lower))
        def _():
            grad_out[0][...] = sum_near(n).astype(BF16)
            remote(grad_out[0], grad_out[0], 5, pair_recv.at[3], me, 0).start()
            wait_sent(kv_out, 5)

        @pl.when(lower)
        def _():
            sum_far()
            with jax.named_scope("w_finsend"):
                wait_sent(grad_out[1], 5)
                wait_sent(part, 2)

    @pl.when(core == 0)
    def _():
        @pl.when(jnp.logical_not(lower))
        def _():
            with jax.named_scope("w_fin"):
                wait_bytes(kv_out, pair_recv.at[3])

        @pl.when(lower)
        def _():
            with jax.named_scope("w_part"):
                wait_bytes(part, pair_recv.at[4])
            sum_far()
            with jax.named_scope("w_finv"):
                wait_bytes(grad_out[1], pair_recv.at[3])


def store_kernel(out_ref, dq_hbm, dk_hbm, dv_hbm, sem):
    start = 0
    for dst in (dq_hbm, dk_hbm, dv_hbm):
        span = pl.ds(start, dst.shape[0])
        pltpu.make_async_copy(out_ref.at[span], dst, sem).start()
        start += dst.shape[0]
    pltpu.make_async_copy(out_ref, out_ref, sem).wait()


def body(n, queries, keys, values, out, log_total, d_out, span_order):
    _, toks, heads, width = queries.shape
    rows = toks * heads
    m = n // 2
    flat = lambda x: x.reshape(rows, width)
    anywhere = pl.BlockSpec(memory_space=pltpu.HBM)
    in_vmem = pl.BlockSpec(memory_space=pltpu.VMEM)
    grads = pl.pallas_call(
        functools.partial(kernel, n, heads),
        out_shape=pltpu.VMEM((rows + 2 * toks, width), BF16),
        in_specs=[anywhere] * 7,
        out_specs=in_vmem,
        scratch_shapes=[
            pltpu.VMEM((2, 2, rows, width), BF16),
            pltpu.VMEM((rows, width), BF16),
            pltpu.VMEM((heads, toks), F32),
            pltpu.VMEM((2, toks, width), BF16),
            pltpu.VMEM((m + 1, 2, toks, width), BF16),
            pltpu.VMEM((2, 8, rows), F32),
            pltpu.VMEM((m, toks, 2 * rows), BF16),
            pltpu.VMEM((m, 2, toks, width), BF16),
            pltpu.VMEM((2, n, toks, width), BF16),
            pltpu.VMEM((toks, width), F32),
            pltpu.VMEM((rows, width), F32),
            pltpu.VMEM((rows, width), F32),
            pltpu.SMEM((span_order.shape[1],), jnp.int32),
            pltpu.SemaphoreType.DMA((6,)),
            pltpu.SemaphoreType.DMA((5,)),
            pltpu.SemaphoreType.DMA((m, 2)),
            pltpu.SemaphoreType.DMA((3,)),
            pltpu.SemaphoreType.DMA((3,)),
            pltpu.SemaphoreType.REGULAR,
        ],
        compiler_params=pltpu.CompilerParams(collective_id=0, has_side_effects=True),
    )(
        flat(queries),
        keys[0],
        values[0],
        flat(out),
        log_total[0],
        flat(d_out),
        span_order[0],
    )
    dq, dk, dv = pl.pallas_call(
        store_kernel,
        out_shape=(
            jax.ShapeDtypeStruct((rows, width), BF16),
            jax.ShapeDtypeStruct((toks, width), BF16),
            jax.ShapeDtypeStruct((toks, width), BF16),
        ),
        in_specs=[in_vmem],
        out_specs=(anywhere,) * 3,
        scratch_shapes=[pltpu.SemaphoreType.DMA],
        compiler_params=pltpu.CompilerParams(vmem_limit_bytes=2**20),
    )(grads)
    return dq.reshape(queries.shape), dk[None], dv[None]


def solution(mesh):
    seq = ("groups", "outer")
    wide = P(seq, "inner", "head", None)
    narrow = P(seq, "inner", None)
    return jax.shard_map(
        functools.partial(body, mesh.shape["inner"]),
        mesh=mesh,
        in_specs=(wide, narrow, narrow, wide, P(seq, "head", "inner"), wide, P(seq, None)),
        out_specs=(wide, narrow, narrow),
        check_vma=False,
    )
```

```python
import functools
import math

import jax
import jax.numpy as jnp
from jax import lax
from jax.experimental import pallas as pl
from jax.experimental.pallas import tpu as pltpu
from jax.sharding import PartitionSpec as P

MESH = pl.DeviceIdType.MESH
F32 = jnp.float32
BF16 = jnp.bfloat16
NT = (((1,), (1,)), ((), ()))
TN = (((0,), (0,)), ((), ()))
LOG2E = math.log2(math.e)


def dot(a, b, dims=(((1,), (0,)), ((), ()))):
    return lax.dot_general(a, b, dims, preferred_element_type=F32)


def kernel(
    n,
    heads,
    q_hbm,
    k_hbm,
    v_hbm,
    o_hbm,
    l_hbm,
    g_hbm,
    order_hbm,
    out_ref,
    qg,
    os_,
    ls,
    mine,
    kv,
    stat,
    ds_all,
    send_buf,
    recv_buf,
    part,
    dq_send,
    dq_recv,
    order,
    sem,
    pair_recv,
    kv_recv,
    grad_recv,
    entry,
    entered,
):
    me = lax.axis_index("inner")
    core = lax.axis_index("head")
    m = n // 2
    split = m + m // 2
    toks, width = kv.shape[2], kv.shape[3]
    half = toks // 2
    rows = qg.shape[2]
    dq_ref, kv_out = out_ref.at[pl.ds(0, rows)], out_ref.at[pl.ds(rows, 2 * toks)]
    grad_out = [out_ref.at[pl.ds(rows + i * toks, toks)] for i in range(2)]
    scale = 1.0 / math.sqrt(width)
    partner = {"head": 1 - core}

    def chip(d):
        at = me
        for k in range(n.bit_length()):
            if d >> k & 1:
                at = at + (1 - 2 * ((me // 2**k) % 2)) * 2**k
        return at

    owners = [chip(j) + core * (chip(n - 1 - j) - chip(j)) for j in range(m)]

    barrier = pltpu.get_barrier_semaphore()

    def greet(inner, head, when=None):
        def signal():
            pl.semaphore_signal(
                barrier, inc=1, device_id={"inner": inner, "head": head}, device_id_type=MESH
            )

        signal() if when is None else pl.when(when)(signal)

    @pl.when(core == 1)
    def _():
        greet(0, 1, me == 1)
        for d in reversed(range(split, n)):
            greet(chip(d), 1, chip(d) != 0)
        for d in reversed(range(m, split)):
            greet(chip(d), 0, chip(d) != 0)
        greet(me, 0)

    @pl.when(core == 0)
    def _():
        for d in range(1, m):
            greet(chip(d), 0, chip(d) != 0)
        greet(me, 1)

    loads = [
        pltpu.make_async_copy(src, dst, sem.at[i])
        for src, dst, i in (
            (k_hbm, mine.at[0], 0),
            (v_hbm, mine.at[1], 0),
            (q_hbm, qg.at[0, 0], 1),
            (g_hbm, qg.at[0, 1], 1),
            (o_hbm, os_, 2),
            (l_hbm, ls, 3),
            (order_hbm, order, 4),
        )
    ]
    for load in loads:
        load.start()

    @pl.when(core == 0)
    def _():
        pltpu.make_async_copy(k_hbm, kv.at[0, 0], kv_recv.at[0, 0]).start()
        pltpu.make_async_copy(v_hbm, kv.at[0, 1], kv_recv.at[0, 1]).start()

    def remote(src, dst, send, recv, inner, head):
        return pltpu.make_async_remote_copy(
            src_ref=src,
            dst_ref=dst,
            send_sem=sem.at[send],
            recv_sem=recv,
            device_id={"inner": inner, "head": head},
            device_id_type=MESH,
        )

    def wait_bytes(ref, recv):
        remote(ref, ref, 0, recv, me, 1 - core).wait_recv()

    def wait_sent(ref, send):
        remote(ref, ref, send, pair_recv.at[0], me, 1 - core).wait_send()

    def slot_of(d):
        return d if d < m else n - 1 - d

    def kv_send(d):
        for i in range(2):
            place = (slot_of(d), i)
            remote(
                mine.at[i], kv.at[place], 0, kv_recv.at[place], chip(d), int(d >= m)
            ).start()

    wait_bytes(mine, sem.at[0])
    sent = jnp.where(
        me == 0,
        core,
        jnp.where(core == 1, n - split, split - 1),
    )
    pl.semaphore_wait(barrier, 1 + sent)

    pieces = [
        ((0, pl.ds(0, half)), entry.at[0]),
        ((0, pl.ds(half, half)), entry.at[1]),
        ((1,), entry.at[2]),
    ]

    @pl.when(me == 0)
    def _():
        @pl.when(core == 1)
        def _():
            for piece, ready in pieces:
                remote(mine.at[piece], kv.at[(m, *piece)], 0, ready, 1, 1).start()

    @pl.when(me != 0)
    def _():
        @pl.when(core == 1)
        def _():
            for d in reversed(range(split, n)):
                kv_send(d)

        @pl.when(core == 0)
        def _():
            @pl.when(me == 1)
            def _():
                pl.semaphore_signal(
                    entered, inc=1, device_id={"inner": me, "head": 1}, device_id_type=MESH
                )

            @pl.when(me == 1)
            def _():
                for d in range(1, m):
                    kv_send(d)

    def middle_sends(when):
        @pl.when(jnp.logical_and(core == 0, when))
        def _():
            for d in range(m, split):
                kv_send(d)

    middle_sends(me > 1)

    @pl.when(jnp.logical_and(core == 0, me > 1))
    def _():
        for d in range(1, m):
            kv_send(d)

    wait_bytes(qg.at[0], sem.at[1])
    remote(qg.at[0], qg.at[1], 1, pair_recv.at[0], me, 1 - core).start()
    loads[4].wait()
    loads[5].wait()

    col = lax.broadcasted_iota(jnp.int32, (toks, rows), 1)
    spread = jnp.where(
        col // heads == lax.broadcasted_iota(jnp.int32, (toks, rows), 0), 1.0, 0.0
    )
    head_of = lax.broadcasted_iota(jnp.int32, (heads, rows), 1) % heads
    pick = head_of == lax.broadcasted_iota(jnp.int32, (heads, rows), 0)
    ones = jnp.ones((8, width), BF16)
    total = jnp.dot(
        ls[...], spread, preferred_element_type=F32, precision=lax.Precision.HIGHEST
    )
    total = jnp.sum(jnp.where(pick, total, 0.0), axis=0, keepdims=True)
    prod = os_[...].astype(F32) * qg[0, 1].astype(F32)
    high = prod.astype(BF16)
    rest = (prod - high.astype(F32)).astype(BF16)
    delta = dot(ones, high, NT) + dot(ones, rest, NT)
    stat[0, 0:1] = total * LOG2E
    stat[0, 1:2] = delta[0:1]
    remote(stat.at[0], stat.at[1], 2, pair_recv.at[1], me, 1 - core).start()

    loads[6].wait()

    relays = jnp.logical_and(me == 1, core == 1)

    @pl.when(relays)
    def _():
        def forward(piece, c):
            place = (slot_of(c), *piece)
            remote(
                kv.at[(m, *piece)], kv.at[place], 4, kv_recv.at[place[:2]], c, int(c >= m)
            ).start()

        greeted = [c for c in range(m, n - 1) if c ^ 1 >= split]
        rest = [c for c in range(1, n - 1) if c not in greeted]
        for piece, ready in pieces[:2]:
            wait_bytes(kv.at[(m, *piece)], ready)
            for c in greeted:
                forward(piece, c)
        pl.semaphore_wait(entered, 1)
        for c in (n - 1, *rest):
            forward((0,), c)
        piece, ready = pieces[2]
        wait_bytes(kv.at[(m, *piece)], ready)
        for c in (*greeted, *rest, n - 1):
            forward(piece, c)

    tok = (lax.broadcasted_iota(jnp.int32, (1, rows), 1)) // heads
    q_span = jnp.where(tok < half, order[2 * me], order[2 * me + 1])
    q_pos = q_span * half + tok % half
    q_span = jnp.concatenate([q_span, q_span], axis=1)
    q_pos = jnp.concatenate([q_pos, q_pos], axis=1)
    key_row = lax.broadcasted_iota(jnp.int32, (toks, 1), 0)

    with jax.named_scope("w_pair"):
        wait_bytes(qg.at[1], pair_recv.at[0])
        wait_bytes(stat.at[1], pair_recv.at[1])
    totals = jnp.concatenate([stat[0, 0:1], stat[1, 0:1]], axis=1)
    deltas = jnp.concatenate([stat[0, 1:2], stat[1, 1:2]], axis=1)

    def by_span(a, b):
        return jnp.where(key_row < half, a, b)

    def block(j):
        spans = [order[2 * owners[j] + h] for h in range(2)]
        queries = qg[:, 0].reshape(2 * rows, width)
        grads = qg[:, 1].reshape(2 * rows, width)
        with jax.named_scope(f"w_k{j}"):
            wait_bytes(kv.at[j, 0], kv_recv.at[j, 0])
        with jax.named_scope(f"dv{j}"):
            scores = dot(kv[j, 0], queries, NT)
            if j == 0:
                visible = by_span(*spans) * half + key_row % half <= q_pos
                probs = jnp.exp2(
                    jnp.where(visible, scores * (scale * LOG2E) - totals, -jnp.inf)
                )
            else:
                shifts = [jnp.where(k_span < q_span, totals, jnp.inf) for k_span in spans]
                probs = jnp.exp2(
                    jnp.concatenate(
                        [
                            scores[h * half : (h + 1) * half] * (scale * LOG2E) - shifts[h]
                            for h in range(2)
                        ]
                    )
                )
            yield 1, dot(probs.astype(BF16), grads)
        with jax.named_scope(f"w_v{j}"):
            wait_bytes(kv.at[j, 1], kv_recv.at[j, 1])
        with jax.named_scope(f"dk{j}"):
            grad_probs = dot(kv[j, 1], grads, NT)
            grad_scores = (probs * (grad_probs - deltas) * scale).astype(BF16)
            ds_all[j] = grad_scores
            yield 0, dot(grad_scores, queries)

    last = jnp.logical_and(core == 1, me == n - 1)
    held = jnp.logical_and(core == 0, me == n - 1)

    def grad_copy(j, i, head=1):
        spare = i == 0
        ready = grad_recv.at[jnp.where(last, 2, 0)] if spare else grad_recv.at[1]
        return remote(
            send_buf.at[j, i], recv_buf.at[i, me], 3 if head else 5, ready, owners[j], head
        )

    for j in range(m):
        for i, grad in block(j):
            send_buf[j, i] = grad.astype(BF16)
            if i == 0:
                pl.when(last)(lambda: grad_copy(j, i, 0).start())
            if j:
                pl.when(jnp.logical_not(held))(lambda: grad_copy(j, i).start())
            else:
                grad_copy(j, i).start()
            if (j, i) == (0, 0):
                middle_sends(me == 1)

    def query_grad(i):
        total = None
        for j in range(m):
            term = dot(ds_all[j, :, i * rows : (i + 1) * rows], kv[j, 0], TN)
            total = term if total is None else total + term
        return total

    pl.when(relays)(lambda: wait_sent(recv_buf.at[:, 0 : n - 1], 4))

    with jax.named_scope("dq"):
        dq_send[...] = query_grad(1)
        dq_copy = remote(dq_send, dq_recv, 4, pair_recv.at[2], me, 1 - core)
        dq_copy.start()
        own_grad = query_grad(0)

    @pl.when(held)
    def _():
        for j in range(1, m):
            for i in (1, 0):
                grad_copy(j, i).start()

    lower = me < m

    def sum_near(count):
        with jax.named_scope("w_near"):
            wait_bytes(recv_buf.at[0, 0:count], grad_recv.at[0])
        return sum(recv_buf[0, c].astype(F32) for c in range(count))

    wait_sent(stat.at[0], 2)

    def finish_values():
        with jax.named_scope("w_v"):
            wait_bytes(recv_buf.at[1], grad_recv.at[1])
        grad_out[1][...] = sum(recv_buf[1, c].astype(F32) for c in range(n)).astype(BF16)
        remote(grad_out[1], grad_out[1], 5, pair_recv.at[3], me, 0).start()

    @pl.when(jnp.logical_and(core == 1, lower))
    def _():
        part[...] = sum_near(n - 1)
        remote(part, part, 2, pair_recv.at[4], me, 0).start()

    pl.when(jnp.logical_and(core == 1, me == 0))(finish_values)

    with jax.named_scope("w_dq"):
        dq_copy.wait_recv()
    dq_ref[...] = (own_grad + dq_recv[...]).astype(BF16)

    with jax.named_scope("w_sends"):
        wait_sent(qg.at[0], 1)
        wait_sent(send_buf, 3)
        dq_copy.wait_send()

        @pl.when(core == 1)
        def _():
            pl.when(me == 0)(lambda: wait_sent(mine, 0))
            pl.when(me != 0)(lambda: wait_sent(recv_buf.at[:, 0 : n - split], 0))

        @pl.when(jnp.logical_and(core == 0, me != 0))
        def _():
            wait_sent(recv_buf.at[:, 1:split], 0)

    def sum_far():
        with jax.named_scope("w_far"):
            wait_bytes(recv_buf.at[0, n - 1], grad_recv.at[2])
        grad_out[0][...] = (part[...] + recv_buf[0, n - 1].astype(F32)).astype(BF16)

    @pl.when(core == 1)
    def _():
        pl.when(last)(lambda: wait_sent(recv_buf.at[0, 0:m], 5))
        pl.when(me != 0)(finish_values)

        @pl.when(jnp.logical_not(lower))
        def _():
            grad_out[0][...] = sum_near(n).astype(BF16)
            remote(grad_out[0], grad_out[0], 5, pair_recv.at[3], me, 0).start()
            wait_sent(kv_out, 5)

        @pl.when(lower)
        def _():
            sum_far()
            with jax.named_scope("w_finsend"):
                wait_sent(grad_out[1], 5)
                wait_sent(part, 2)

    @pl.when(core == 0)
    def _():
        @pl.when(jnp.logical_not(lower))
        def _():
            with jax.named_scope("w_fin"):
                wait_bytes(kv_out, pair_recv.at[3])

        @pl.when(lower)
        def _():
            with jax.named_scope("w_part"):
                wait_bytes(part, pair_recv.at[4])
            sum_far()
            with jax.named_scope("w_finv"):
                wait_bytes(grad_out[1], pair_recv.at[3])


def store_kernel(out_ref, dq_hbm, dk_hbm, dv_hbm, sem):
    start = 0
    for dst in (dq_hbm, dk_hbm, dv_hbm):
        span = pl.ds(start, dst.shape[0])
        pltpu.make_async_copy(out_ref.at[span], dst, sem).start()
        start += dst.shape[0]
    pltpu.make_async_copy(out_ref, out_ref, sem).wait()


def body(n, queries, keys, values, out, log_total, d_out, span_order):
    _, toks, heads, width = queries.shape
    rows = toks * heads
    m = n // 2
    flat = lambda x: x.reshape(rows, width)
    anywhere = pl.BlockSpec(memory_space=pltpu.HBM)
    in_vmem = pl.BlockSpec(memory_space=pltpu.VMEM)
    grads = pl.pallas_call(
        functools.partial(kernel, n, heads),
        out_shape=pltpu.VMEM((rows + 2 * toks, width), BF16),
        in_specs=[anywhere] * 7,
        out_specs=in_vmem,
        scratch_shapes=[
            pltpu.VMEM((2, 2, rows, width), BF16),
            pltpu.VMEM((rows, width), BF16),
            pltpu.VMEM((heads, toks), F32),
            pltpu.VMEM((2, toks, width), BF16),
            pltpu.VMEM((m + 1, 2, toks, width), BF16),
            pltpu.VMEM((2, 8, rows), F32),
            pltpu.VMEM((m, toks, 2 * rows), BF16),
            pltpu.VMEM((m, 2, toks, width), BF16),
            pltpu.VMEM((2, n, toks, width), BF16),
            pltpu.VMEM((toks, width), F32),
            pltpu.VMEM((rows, width), F32),
            pltpu.VMEM((rows, width), F32),
            pltpu.SMEM((span_order.shape[1],), jnp.int32),
            pltpu.SemaphoreType.DMA((6,)),
            pltpu.SemaphoreType.DMA((5,)),
            pltpu.SemaphoreType.DMA((m, 2)),
            pltpu.SemaphoreType.DMA((3,)),
            pltpu.SemaphoreType.DMA((3,)),
            pltpu.SemaphoreType.REGULAR,
        ],
        compiler_params=pltpu.CompilerParams(collective_id=0, has_side_effects=True),
    )(
        flat(queries),
        keys[0],
        values[0],
        flat(out),
        log_total[0],
        flat(d_out),
        span_order[0],
    )
    dq, dk, dv = pl.pallas_call(
        store_kernel,
        out_shape=(
            jax.ShapeDtypeStruct((rows, width), BF16),
            jax.ShapeDtypeStruct((toks, width), BF16),
            jax.ShapeDtypeStruct((toks, width), BF16),
        ),
        in_specs=[in_vmem],
        out_specs=(anywhere,) * 3,
        scratch_shapes=[pltpu.SemaphoreType.DMA],
        compiler_params=pltpu.CompilerParams(vmem_limit_bytes=2**20),
    )(grads)
    return dq.reshape(queries.shape), dk[None], dv[None]


def solution(mesh):
    seq = ("groups", "outer")
    wide = P(seq, "inner", "head", None)
    narrow = P(seq, "inner", None)
    return jax.shard_map(
        functools.partial(body, mesh.shape["inner"]),
        mesh=mesh,
        in_specs=(wide, narrow, narrow, wide, P(seq, "head", "inner"), wide, P(seq, None)),
        out_specs=(wide, narrow, narrow),
        check_vma=False,
    )
```

```python
import functools
import math

import jax
import jax.numpy as jnp
from jax import lax
from jax.experimental import pallas as pl
from jax.experimental.pallas import tpu as pltpu
from jax.sharding import PartitionSpec as P

MESH = pl.DeviceIdType.MESH
F32 = jnp.float32
BF16 = jnp.bfloat16
NT = (((1,), (1,)), ((), ()))
TN = (((0,), (0,)), ((), ()))
LOG2E = math.log2(math.e)


def dot(a, b, dims=(((1,), (0,)), ((), ()))):
    return lax.dot_general(a, b, dims, preferred_element_type=F32)


def kernel(
    n,
    heads,
    q_hbm,
    k_hbm,
    v_hbm,
    o_hbm,
    l_hbm,
    g_hbm,
    order_hbm,
    out_ref,
    qg,
    os_,
    ls,
    mine,
    kv,
    stat,
    ds_all,
    send_buf,
    recv_buf,
    part,
    dq_send,
    dq_recv,
    order,
    sem,
    pair_recv,
    kv_recv,
    grad_recv,
    entry,
    entered,
):
    me = lax.axis_index("inner")
    core = lax.axis_index("head")
    m = n // 2
    split = m + m // 2
    toks, width = kv.shape[2], kv.shape[3]
    half = toks // 2
    rows = qg.shape[2]
    dq_ref, kv_out = out_ref.at[pl.ds(0, rows)], out_ref.at[pl.ds(rows, 2 * toks)]
    grad_out = [out_ref.at[pl.ds(rows + i * toks, toks)] for i in range(2)]
    scale = 1.0 / math.sqrt(width)
    partner = {"head": 1 - core}

    def chip(d):
        at = me
        for k in range(n.bit_length()):
            if d >> k & 1:
                at = at + (1 - 2 * ((me // 2**k) % 2)) * 2**k
        return at

    owners = [chip(j) + core * (chip(n - 1 - j) - chip(j)) for j in range(m)]

    barrier = pltpu.get_barrier_semaphore()

    def greet(inner, head, when=None):
        def signal():
            pl.semaphore_signal(
                barrier, inc=1, device_id={"inner": inner, "head": head}, device_id_type=MESH
            )

        signal() if when is None else pl.when(when)(signal)

    @pl.when(core == 1)
    def _():
        greet(0, 1, me == 1)
        for d in reversed(range(split, n)):
            greet(chip(d), 1, chip(d) != 0)
        for d in reversed(range(m, split)):
            greet(chip(d), 0, chip(d) != 0)
        greet(me, 0)

    @pl.when(core == 0)
    def _():
        for d in range(1, m):
            greet(chip(d), 0, chip(d) != 0)
        greet(me, 1)

    loads = [
        pltpu.make_async_copy(src, dst, sem.at[i])
        for src, dst, i in (
            (k_hbm, mine.at[0], 0),
            (v_hbm, mine.at[1], 0),
            (q_hbm, qg.at[0, 0], 1),
            (g_hbm, qg.at[0, 1], 1),
            (o_hbm, os_, 2),
            (l_hbm, ls, 3),
            (order_hbm, order, 4),
        )
    ]
    for load in loads:
        load.start()

    @pl.when(core == 0)
    def _():
        pltpu.make_async_copy(k_hbm, kv.at[0, 0], kv_recv.at[0, 0]).start()
        pltpu.make_async_copy(v_hbm, kv.at[0, 1], kv_recv.at[0, 1]).start()

    def remote(src, dst, send, recv, inner, head):
        return pltpu.make_async_remote_copy(
            src_ref=src,
            dst_ref=dst,
            send_sem=sem.at[send],
            recv_sem=recv,
            device_id={"inner": inner, "head": head},
            device_id_type=MESH,
        )

    def wait_bytes(ref, recv):
        remote(ref, ref, 0, recv, me, 1 - core).wait_recv()

    def wait_sent(ref, send):
        remote(ref, ref, send, pair_recv.at[0], me, 1 - core).wait_send()

    def slot_of(d):
        return d if d < m else n - 1 - d

    def kv_send(d):
        for i in range(2):
            place = (slot_of(d), i)
            remote(
                mine.at[i], kv.at[place], 0, kv_recv.at[place], chip(d), int(d >= m)
            ).start()

    wait_bytes(mine, sem.at[0])
    sent = jnp.where(
        me == 0,
        core,
        jnp.where(core == 1, n - split, split - 1),
    )
    pl.semaphore_wait(barrier, 1 + sent)

    pieces = [
        ((0, pl.ds(0, half)), entry.at[0]),
        ((0, pl.ds(half, half)), entry.at[1]),
        ((1,), entry.at[2]),
    ]

    @pl.when(me == 0)
    def _():
        @pl.when(core == 1)
        def _():
            for piece, ready in pieces:
                remote(mine.at[piece], kv.at[(m, *piece)], 0, ready, 1, 1).start()

    @pl.when(me != 0)
    def _():
        @pl.when(core == 1)
        def _():
            for d in reversed(range(split, n)):
                kv_send(d)

        @pl.when(core == 0)
        def _():
            @pl.when(me == 1)
            def _():
                pl.semaphore_signal(
                    entered, inc=1, device_id={"inner": me, "head": 1}, device_id_type=MESH
                )

            @pl.when(me == 1)
            def _():
                for d in range(1, m):
                    kv_send(d)

    def middle_sends(when):
        @pl.when(jnp.logical_and(core == 0, when))
        def _():
            for d in range(m, split):
                kv_send(d)

    middle_sends(me > 1)

    @pl.when(jnp.logical_and(core == 0, me > 1))
    def _():
        for d in range(1, m):
            kv_send(d)

    wait_bytes(qg.at[0], sem.at[1])
    remote(qg.at[0], qg.at[1], 1, pair_recv.at[0], me, 1 - core).start()
    loads[4].wait()
    loads[5].wait()

    col = lax.broadcasted_iota(jnp.int32, (toks, rows), 1)
    spread = jnp.where(
        col // heads == lax.broadcasted_iota(jnp.int32, (toks, rows), 0), 1.0, 0.0
    )
    head_of = lax.broadcasted_iota(jnp.int32, (heads, rows), 1) % heads
    pick = head_of == lax.broadcasted_iota(jnp.int32, (heads, rows), 0)
    ones = jnp.ones((8, width), BF16)
    total = jnp.dot(
        ls[...], spread, preferred_element_type=F32, precision=lax.Precision.HIGHEST
    )
    total = jnp.sum(jnp.where(pick, total, 0.0), axis=0, keepdims=True)
    prod = os_[...].astype(F32) * qg[0, 1].astype(F32)
    high = prod.astype(BF16)
    rest = (prod - high.astype(F32)).astype(BF16)
    delta = dot(ones, high, NT) + dot(ones, rest, NT)
    stat[0, 0:1] = total * LOG2E
    stat[0, 1:2] = delta[0:1]
    remote(stat.at[0], stat.at[1], 2, pair_recv.at[1], me, 1 - core).start()

    loads[6].wait()

    relays = jnp.logical_and(me == 1, core == 1)

    @pl.when(relays)
    def _():
        def forward(piece, c):
            place = (slot_of(c), *piece)
            remote(
                kv.at[(m, *piece)], kv.at[place], 4, kv_recv.at[place[:2]], c, int(c >= m)
            ).start()

        greeted = [c for c in range(m, n - 1) if c ^ 1 >= split]
        rest = [c for c in range(1, n - 1) if c not in greeted]
        for piece, ready in pieces[:2]:
            wait_bytes(kv.at[(m, *piece)], ready)
            for c in greeted:
                forward(piece, c)
        pl.semaphore_wait(entered, 1)
        for c in (n - 1, *rest):
            forward((0,), c)
        piece, ready = pieces[2]
        wait_bytes(kv.at[(m, *piece)], ready)
        for c in (*greeted, *rest, n - 1):
            forward(piece, c)

    tok = (lax.broadcasted_iota(jnp.int32, (1, rows), 1)) // heads
    q_span = jnp.where(tok < half, order[2 * me], order[2 * me + 1])
    q_pos = q_span * half + tok % half
    q_span = jnp.concatenate([q_span, q_span], axis=1)
    q_pos = jnp.concatenate([q_pos, q_pos], axis=1)
    key_row = lax.broadcasted_iota(jnp.int32, (toks, 1), 0)

    with jax.named_scope("w_pair"):
        wait_bytes(qg.at[1], pair_recv.at[0])
        wait_bytes(stat.at[1], pair_recv.at[1])
    totals = jnp.concatenate([stat[0, 0:1], stat[1, 0:1]], axis=1)
    deltas = jnp.concatenate([stat[0, 1:2], stat[1, 1:2]], axis=1)

    def by_span(a, b):
        return jnp.where(key_row < half, a, b)

    def block(j):
        spans = [order[2 * owners[j] + h] for h in range(2)]
        queries = qg[:, 0].reshape(2 * rows, width)
        grads = qg[:, 1].reshape(2 * rows, width)
        with jax.named_scope(f"w_k{j}"):
            wait_bytes(kv.at[j, 0], kv_recv.at[j, 0])
        with jax.named_scope(f"dv{j}"):
            scores = dot(kv[j, 0], queries, NT)
            if j == 0:
                visible = by_span(*spans) * half + key_row % half <= q_pos
                probs = jnp.exp2(
                    jnp.where(visible, scores * (scale * LOG2E) - totals, -jnp.inf)
                )
            else:
                shifts = [jnp.where(k_span < q_span, totals, jnp.inf) for k_span in spans]
                probs = jnp.exp2(
                    jnp.concatenate(
                        [
                            scores[h * half : (h + 1) * half] * (scale * LOG2E) - shifts[h]
                            for h in range(2)
                        ]
                    )
                )
            scaled = probs * scale
            yield 1, slice(0, toks), dot(probs.astype(BF16), grads)
        with jax.named_scope(f"w_v{j}"):
            wait_bytes(kv.at[j, 1], kv_recv.at[j, 1])
        with jax.named_scope(f"dk{j}"):
            grad_probs = dot(kv[j, 1], grads, NT)
            grad_scores = (scaled * (grad_probs - deltas)).astype(BF16)
            ds_all[j] = grad_scores
            for span in (slice(0, half), slice(half, toks)):
                yield 0, span, dot(grad_scores[span], queries)

    last = jnp.logical_and(core == 1, me == n - 1)
    held = jnp.logical_and(core == 0, me == n - 1)

    def grad_copy(j, i, head=1, span=slice(0, None)):
        rows_of = pl.ds(span.start, (span.stop or toks) - span.start)
        spare = i == 0
        ready = grad_recv.at[jnp.where(last, 2, 0)] if spare else grad_recv.at[1]
        return remote(
            send_buf.at[j, i, rows_of],
            recv_buf.at[i, me, rows_of],
            3 if head else 5,
            ready,
            owners[j],
            head,
        )

    for j in range(m):
        for i, span, grad in block(j):
            send_buf[j, i, span] = grad.astype(BF16)
            if i == 0:
                pl.when(last)(lambda: grad_copy(j, i, 0, span).start())
                if span.stop < toks:
                    continue
            if j:
                pl.when(jnp.logical_not(held))(lambda: grad_copy(j, i).start())
            else:
                grad_copy(j, i).start()
            if (j, i) == (0, 0):
                middle_sends(me == 1)

    def query_grad(i):
        total = None
        for j in range(m):
            term = dot(ds_all[j, :, i * rows : (i + 1) * rows], kv[j, 0], TN)
            total = term if total is None else total + term
        return total

    pl.when(relays)(lambda: wait_sent(recv_buf.at[:, 0 : n - 1], 4))

    with jax.named_scope("dq"):
        dq_send[...] = query_grad(1)
        dq_copy = remote(dq_send, dq_recv, 4, pair_recv.at[2], me, 1 - core)
        dq_copy.start()
        own_grad = query_grad(0)

    @pl.when(held)
    def _():
        for j in range(1, m):
            for i in (1, 0):
                grad_copy(j, i).start()

    lower = me < m

    def sum_near(count):
        with jax.named_scope("w_near"):
            wait_bytes(recv_buf.at[0, 0:count], grad_recv.at[0])
        return sum(recv_buf[0, c].astype(F32) for c in range(count))

    wait_sent(stat.at[0], 2)

    def finish_values():
        with jax.named_scope("w_v"):
            wait_bytes(recv_buf.at[1], grad_recv.at[1])
        grad_out[1][...] = sum(recv_buf[1, c].astype(F32) for c in range(n)).astype(BF16)
        remote(grad_out[1], grad_out[1], 5, pair_recv.at[3], me, 0).start()

    @pl.when(jnp.logical_and(core == 1, lower))
    def _():
        part[...] = sum_near(n - 1)
        remote(part, part, 2, pair_recv.at[4], me, 0).start()

    pl.when(jnp.logical_and(core == 1, me == 0))(finish_values)

    with jax.named_scope("w_dq"):
        dq_copy.wait_recv()
    dq_ref[...] = (own_grad + dq_recv[...]).astype(BF16)

    with jax.named_scope("w_sends"):
        wait_sent(qg.at[0], 1)
        wait_sent(send_buf, 3)
        dq_copy.wait_send()

        @pl.when(core == 1)
        def _():
            pl.when(me == 0)(lambda: wait_sent(mine, 0))
            pl.when(me != 0)(lambda: wait_sent(recv_buf.at[:, 0 : n - split], 0))

        @pl.when(jnp.logical_and(core == 0, me != 0))
        def _():
            wait_sent(recv_buf.at[:, 1:split], 0)

    def sum_far():
        with jax.named_scope("w_far"):
            wait_bytes(recv_buf.at[0, n - 1], grad_recv.at[2])
        grad_out[0][...] = (part[...] + recv_buf[0, n - 1].astype(F32)).astype(BF16)

    @pl.when(core == 1)
    def _():
        pl.when(last)(lambda: wait_sent(recv_buf.at[0, 0:m], 5))
        pl.when(me != 0)(finish_values)

        @pl.when(jnp.logical_not(lower))
        def _():
            grad_out[0][...] = sum_near(n).astype(BF16)
            remote(grad_out[0], grad_out[0], 5, pair_recv.at[3], me, 0).start()
            wait_sent(kv_out, 5)

        @pl.when(lower)
        def _():
            sum_far()
            with jax.named_scope("w_finsend"):
                wait_sent(grad_out[1], 5)
                wait_sent(part, 2)

    @pl.when(core == 0)
    def _():
        @pl.when(jnp.logical_not(lower))
        def _():
            with jax.named_scope("w_fin"):
                wait_bytes(kv_out, pair_recv.at[3])

        @pl.when(lower)
        def _():
            with jax.named_scope("w_part"):
                wait_bytes(part, pair_recv.at[4])
            sum_far()
            with jax.named_scope("w_finv"):
                wait_bytes(grad_out[1], pair_recv.at[3])


def store_kernel(out_ref, dq_hbm, dk_hbm, dv_hbm, sem):
    start = 0
    for dst in (dq_hbm, dk_hbm, dv_hbm):
        span = pl.ds(start, dst.shape[0])
        pltpu.make_async_copy(out_ref.at[span], dst, sem).start()
        start += dst.shape[0]
    pltpu.make_async_copy(out_ref, out_ref, sem).wait()


def body(n, queries, keys, values, out, log_total, d_out, span_order):
    _, toks, heads, width = queries.shape
    rows = toks * heads
    m = n // 2
    flat = lambda x: x.reshape(rows, width)
    anywhere = pl.BlockSpec(memory_space=pltpu.HBM)
    in_vmem = pl.BlockSpec(memory_space=pltpu.VMEM)
    grads = pl.pallas_call(
        functools.partial(kernel, n, heads),
        out_shape=pltpu.VMEM((rows + 2 * toks, width), BF16),
        in_specs=[anywhere] * 7,
        out_specs=in_vmem,
        scratch_shapes=[
            pltpu.VMEM((2, 2, rows, width), BF16),
            pltpu.VMEM((rows, width), BF16),
            pltpu.VMEM((heads, toks), F32),
            pltpu.VMEM((2, toks, width), BF16),
            pltpu.VMEM((m + 1, 2, toks, width), BF16),
            pltpu.VMEM((2, 8, rows), F32),
            pltpu.VMEM((m, toks, 2 * rows), BF16),
            pltpu.VMEM((m, 2, toks, width), BF16),
            pltpu.VMEM((2, n, toks, width), BF16),
            pltpu.VMEM((toks, width), F32),
            pltpu.VMEM((rows, width), F32),
            pltpu.VMEM((rows, width), F32),
            pltpu.SMEM((span_order.shape[1],), jnp.int32),
            pltpu.SemaphoreType.DMA((6,)),
            pltpu.SemaphoreType.DMA((5,)),
            pltpu.SemaphoreType.DMA((m, 2)),
            pltpu.SemaphoreType.DMA((3,)),
            pltpu.SemaphoreType.DMA((3,)),
            pltpu.SemaphoreType.REGULAR,
        ],
        compiler_params=pltpu.CompilerParams(collective_id=0, has_side_effects=True),
    )(
        flat(queries),
        keys[0],
        values[0],
        flat(out),
        log_total[0],
        flat(d_out),
        span_order[0],
    )
    dq, dk, dv = pl.pallas_call(
        store_kernel,
        out_shape=(
            jax.ShapeDtypeStruct((rows, width), BF16),
            jax.ShapeDtypeStruct((toks, width), BF16),
            jax.ShapeDtypeStruct((toks, width), BF16),
        ),
        in_specs=[in_vmem],
        out_specs=(anywhere,) * 3,
        scratch_shapes=[pltpu.SemaphoreType.DMA],
        compiler_params=pltpu.CompilerParams(vmem_limit_bytes=2**20),
    )(grads)
    return dq.reshape(queries.shape), dk[None], dv[None]


def solution(mesh):
    seq = ("groups", "outer")
    wide = P(seq, "inner", "head", None)
    narrow = P(seq, "inner", None)
    return jax.shard_map(
        functools.partial(body, mesh.shape["inner"]),
        mesh=mesh,
        in_specs=(wide, narrow, narrow, wide, P(seq, "head", "inner"), wide, P(seq, None)),
        out_specs=(wide, narrow, narrow),
        check_vma=False,
    )
```
